128 devices in a mesh: bank: 8 (over x, core), lane: 16 (over z, y).
Axes of the slice: x: 4, y: 4, z: 4, core: 2. Of those that a mesh axis runs over, the one named last changes fastest.
Arguments:
- amplitudes: float32 [2, 2048, 128, 128], P(None, ('bank', 'lane')), may hold values from -6 to 6
- energies: float32 [2048, 128, 128], P(('bank', 'lane')), may hold values from -2 to 2
- diagonal_angles: float32 [2, 128], replicated, may hold values from 0.3 to 1.2
- turn_angles: float32 [2, 4], replicated, may hold values from 0.3 to 1.2
Outputs:
- state_after: float32 [2, 2048, 128, 128], P(None, ('bank', 'lane'))
The draws below stay inside these ranges and needn't reach their ends.
All inputs are finite; a program needn't handle non-finite values.
Results may differ from the reference program's by a relative error of at most 0.0003.
Values sent between devices are 32-bit elements; how exact they have to be, the bound alone decides.
No kernel may reach another device: no remote copies, remote signals or barrier semaphores. Data moves between devices by JAX's collectives and lax.ppermute only.
A program may use at most 64 MiB of HBM per device.

```python
import jax
import jax.numpy as jnp
from jax import lax

BLOCKS_DEV = 16
ROWS = 128
LANES = 128
BLOCKS = 2048
LAYERS = 2
N_BANK = 8
N_LANE = 16


def shard_levels(key, dims, cuts, smallest, high):
    def one(axis_at, blocks):
        heights = jax.random.uniform(jax.random.fold_in(jax.random.fold_in(key, 6), axis_at), (blocks,), jnp.float32, smallest / len(cuts), high / len(cuts))
        return jnp.repeat(jnp.exp(heights), dims[axis_at] // blocks).reshape((-1,) + (1,) * (len(dims) - axis_at - 1))

    loudness = one(*cuts[0])
    for cut in cuts[1:]:
        loudness = loudness * one(*cut)
    return loudness


def gaussian(own_key, extent, width, most, cuts=(), held_as=jnp.bfloat16):
    drawn = width * jax.random.normal(own_key, extent, jnp.float32)
    if cuts:
        drawn = drawn * shard_levels(own_key, extent, cuts, -0.22, 0.18)
    return jnp.clip(drawn, -most, most).astype(held_as)


def setup_inputs(seed: int = 0) -> dict:
    splits = jax.random.split(jax.random.key(seed), 5)
    amplitudes = gaussian(splits[0], (2, BLOCKS, ROWS, LANES), 1.0, 6.0, ((1, 128),), jnp.float32)
    energies = jnp.clip(jax.random.uniform(splits[1], (BLOCKS, ROWS, LANES), jnp.float32, -2.0, 2.0) * shard_levels(splits[1], (BLOCKS, ROWS, LANES), ((0, 128),), -0.4, 0.0), -2.0, 2.0)
    diagonal_angles = jnp.clip(jax.random.uniform(splits[2], (LAYERS, LANES), jnp.float32, 0.3, 1.2), 0.3, 1.2)
    turn_angles = jnp.clip(jax.random.uniform(splits[3], (LAYERS, 4), jnp.float32, 0.3, 1.2), 0.3, 1.2)
    return {"amplitudes": amplitudes, "energies": energies, "diagonal_angles": diagonal_angles, "turn_angles": turn_angles}


def count_bits(values, count):
    places = jnp.arange(count.bit_length() - 1, dtype=jnp.int32)
    return jnp.sum((values[..., None] >> places) & 1, axis=-1)


def plane_table(count, angle):
    rank = jnp.arange(count, dtype=jnp.int32)
    apart = count_bits(rank[:, None] ^ rank[None, :], count)
    minus = count_bits(rank[:, None] & (rank[:, None] ^ rank[None, :]), count)
    bits = count.bit_length() - 1
    size = jnp.cos(angle) ** (bits - apart).astype(jnp.float32) * jnp.sin(angle) ** apart.astype(jnp.float32)
    return size * jnp.where(minus % 2 == 1, -1.0, 1.0).astype(jnp.float32)


def mix_dim(values, dim, angle):
    real_part = plane_table(values.shape[dim], angle)
    def times(table):
        moved = jnp.tensordot(values, table, axes=([dim], [0]), precision=lax.Precision.HIGHEST)
        return jnp.moveaxis(moved, -1, dim)
    return times(real_part)


def phase_step(values, levels, angle):
    turn = angle * levels
    return jnp.stack([values[0] * jnp.cos(turn) + values[1] * jnp.sin(turn), values[1] * jnp.cos(turn) - values[0] * jnp.sin(turn)])


def reference(amplitudes, energies, diagonal_angles, turn_angles):
    values = amplitudes
    for layer in range(LAYERS):
        values = phase_step(values, energies, diagonal_angles[layer])
        values = mix_dim(values, 3, turn_angles[layer, 0])
        values = mix_dim(values, 2, turn_angles[layer, 1])
        parts = values.reshape(2, N_BANK, N_LANE, BLOCKS_DEV, ROWS, LANES)
        parts = mix_dim(parts, 1, turn_angles[layer, 2])
        parts = mix_dim(parts, 2, turn_angles[layer, 3])
        parts = mix_dim(parts, 3, turn_angles[layer, 2])
        values = parts.reshape(values.shape)
    return values
```

```python
import functools

import jax
import jax.numpy as jnp
import numpy as np
from jax import lax
from jax.experimental import pallas as pl
from jax.experimental.pallas import tpu as pltpu
from jax.sharding import Mesh
from jax.sharding import PartitionSpec as P

AXES = ("x", "c", "z", "y")
XZY = ("x", "z", "y")
VMEM = pltpu.VMEM
SMEM = pltpu.SMEM
TILES = 256
COS0, SIN0, SCALE, TAN1, TAN2, TAN3, TANC = range(7)


def fit(fn, terms, most=5.77):
    k = np.arange(400)
    s = most / 2 * (1 + np.cos(np.pi * (k + 0.5) / 400))
    series = np.polynomial.Chebyshev.fit(s, fn(np.sqrt(s)), terms - 1, domain=[0, most])
    return [float(c) for c in series.convert(kind=np.polynomial.Polynomial).coef]


COS = fit(np.cos, 8)
SIN = fit(lambda t: np.sinc(t / np.pi), 7)


def horner(coef, s):
    total = s * coef[-1] + coef[-2]
    for c in coef[-3::-1]:
        total = total * s + c
    return total


def phase(re, im, level, angle):
    turn = level * angle
    square = turn * turn
    cos = horner(COS, square)
    sin = horner(SIN, square) * turn
    return re * cos + im * sin, im * cos - re * sin


def rotate(tiles, bit, tan):
    step = 1 << bit
    out = list(tiles)
    for i, u in enumerate(tiles):
        if not i & step:
            v = tiles[i + step]
            out[i] = u - tan * v
            out[i + step] = v + tan * u
    return out


def rotate_sublanes(tiles, tan):
    place = lax.broadcasted_iota(jnp.int32, (8, 128), 0)
    for bit in range(3):
        step = 1 << bit
        one = (place & step) != 0
        weight = jnp.where(one, tan, -tan)
        out = []
        for t in tiles:
            below = pltpu.roll(t, step, 0)
            if step == 4:
                other = below
            else:
                other = jnp.where(one, below, pltpu.roll(t, 8 - step, 0))
            out.append(t + weight * other)
        tiles = out
    return tiles


def lane_table(scalars, layer):
    row = lax.broadcasted_iota(jnp.int32, (128, 128), 0)
    col = lax.broadcasted_iota(jnp.int32, (128, 128), 1)
    cos, sin = scalars[layer, COS0], scalars[layer, SIN0]
    table = jnp.full((128, 128), scalars[layer, SCALE], jnp.float32)
    for bit in range(7):
        a, b = (row >> bit) & 1, (col >> bit) & 1
        table = table * jnp.where(a == b, cos, jnp.where(b == 1, sin, -sin))
    high = table.astype(jnp.bfloat16)
    low = (table - high.astype(jnp.float32)).astype(jnp.bfloat16)
    return high, low


def store_table(scalars, layer, table_ref):
    high, low = lane_table(scalars, layer)
    table_ref[0:128, 0:128] = high
    table_ref[0:128, 128:256] = low
    table_ref[128:256, 0:128] = high
    table_ref[128:256, 128:256] = jnp.zeros_like(high)


def mix_lanes(tiles, table_ref):
    rows = jnp.concatenate(tiles, axis=0)
    high = rows.astype(jnp.bfloat16)
    low = (rows - high.astype(jnp.float32)).astype(jnp.bfloat16)
    both = jnp.dot(
        jnp.concatenate([high, low], axis=1), table_ref[...], preferred_element_type=jnp.float32
    )
    mixed = both[:, 0:128] + both[:, 128:256]
    return [mixed[8 * i : 8 * i + 8] for i in range(len(tiles))]


def first_kernel(scalars, state, levels, angle, out):
    tan = scalars[0, TAN2]

    @pl.loop(0, 32)
    def _(j):
        re, im = [], []
        for i in range(8):
            a, b = phase(state[0, 32 * i + j], state[1, 32 * i + j], levels[32 * i + j], angle[...])
            re.append(a)
            im.append(b)
        for p, tiles in enumerate((re, im)):
            for bit in range(3):
                tiles = rotate(tiles, bit, tan)
            for i in range(8):
                out[p, 32 * i + j] = tiles[i]


def second_kernel(scalars, own, other, out, table_ref):
    store_table(scalars, 0, table_ref)
    tan_core, tan_row, tan_block = scalars[0, TANC], scalars[0, TAN1], scalars[0, TAN2]

    @pl.loop(0, 8)
    def _(b):
        for p in range(2):
            tiles = [own[p, 32 * b + i] + tan_core * other[p, 32 * b + i] for i in range(32)]
            tiles = mix_lanes(tiles, table_ref)
            for bit, tan in ((4, tan_block), (3, tan_row), (2, tan_row), (1, tan_row), (0, tan_row)):
                tiles = rotate(tiles, bit, tan)
            tiles = rotate_sublanes(tiles, tan_row)
            for i in range(32):
                out[8 * b + i // 4, p, i % 4] = tiles[i]


def third_kernel(scalars, state, levels, angle, out, table_ref, held):
    store_table(scalars, 1, table_ref)
    x0, zy0 = scalars[0, TAN2], scalars[0, TAN3]
    zy1, row1 = scalars[1, TAN3], scalars[1, TAN1]

    @pl.loop(0, 8)
    def _(g):
        for p in range(2):
            for r in range(4):
                tiles = [state[8 * i + g, p, r] for i in range(8)]
                for bit, tan in ((2, x0), (1, x0), (0, zy0)):
                    tiles = rotate(tiles, bit, tan)
                for i in range(8):
                    held[p, 32 * i + 4 * g + r] = tiles[i]

    @pl.loop(0, 8)
    def _(b):
        parts = [[None] * 32, [None] * 32]
        for r in range(4):
            two = []
            for p in range(2):
                tiles = [held[p, 32 * b + 4 * i + r] for i in range(8)]
                for bit in range(3):
                    tiles = rotate(tiles, bit, zy0)
                two.append(tiles)
            for i in range(8):
                level = levels[32 * b + 4 * i + r]
                parts[0][4 * i + r], parts[1][4 * i + r] = phase(two[0][i], two[1][i], level, angle[...])
        for p in range(2):
            tiles = mix_lanes(parts[p], table_ref)
            for bit, tan in ((4, zy1), (3, zy1), (2, zy1), (1, row1), (0, row1)):
                tiles = rotate(tiles, bit, tan)
            tiles = rotate_sublanes(tiles, row1)
            for i in range(32):
                out[p, 32 * b + i] = tiles[i]


def fourth_kernel(scalars, own, other, out):
    core, x1, zy1 = scalars[1, TANC], scalars[1, TAN2], scalars[1, TAN3]

    @pl.loop(0, 8)
    def _(g):
        for p in range(2):
            for r in range(4):
                at = 4 * g + r
                tiles = [own[p, 32 * i + at] + core * other[p, 32 * i + at] for i in range(8)]
                for bit, tan in ((2, x1), (1, x1), (0, zy1)):
                    tiles = rotate(tiles, bit, tan)
                for i in range(8):
                    out[8 * i + g, p, r] = tiles[i]


def fifth_kernel(scalars, state, out, held):
    block, row = scalars[1, TAN2], scalars[1, TAN1]

    @pl.loop(0, 8)
    def _(g):
        for p in range(2):
            for r in range(4):
                tiles = [state[8 * i + g, p, r] for i in range(8)]
                for bit in range(3):
                    tiles = rotate(tiles, bit, block)
                for i in range(8):
                    held[p, 32 * i + 4 * g + r] = tiles[i]

    @pl.loop(0, 8)
    def _(b):
        for p in range(2):
            for r in range(4):
                tiles = [held[p, 32 * b + 4 * i + r] for i in range(8)]
                for bit, tan in ((2, block), (1, row), (0, row)):
                    tiles = rotate(tiles, bit, tan)
                for i in range(8):
                    out[p, 32 * b + 4 * i + r] = tiles[i]


HOME = (2, TILES, 8, 128)
AWAY = (64, 2, 4, 8, 128)


def call(kernel, name, shape, inputs, scratch=(), flops=20_000_000):
    spaces = [pl.BlockSpec(memory_space=SMEM)] + [pl.BlockSpec(memory_space=VMEM)] * (len(inputs) - 1)
    return pl.pallas_call(
        kernel,
        out_shape=jax.ShapeDtypeStruct(shape, jnp.float32),
        in_specs=spaces,
        out_specs=pl.BlockSpec(memory_space=VMEM),
        scratch_shapes=list(scratch),
        name=name,
        cost_estimate=pl.CostEstimate(flops=flops, bytes_accessed=5 << 20, transcendentals=0),
        compiler_params=pltpu.CompilerParams(vmem_limit_bytes=24 << 20),
    )(*inputs)


def swap_core(state):
    return lax.ppermute(state, "c", [(0, 1), (1, 0)])


def exchange(state):
    return lax.all_to_all(state, XZY, 0, 0, tiled=True)


def layer_scalars(turn_angles):
    cos, sin = jnp.cos(turn_angles), jnp.sin(turn_angles)
    tan = sin / cos
    scale = (cos[:, 1] * cos[:, 2]) ** 7 * cos[:, 3] ** 4
    core = jnp.where(lax.axis_index("c") == 1, tan[:, 2], -tan[:, 2])
    return jnp.stack([cos[:, 0], sin[:, 0], scale, tan[:, 1], tan[:, 2], tan[:, 3], core, core], axis=1)


def body(amplitudes, energies, diagonal_angles, turn_angles):
    scalars = layer_scalars(turn_angles)
    state = amplitudes.reshape(HOME)
    levels = energies.reshape(TILES, 8, 128)
    away_levels = exchange(energies.reshape(64, 32, 128)).reshape(TILES, 8, 128)
    table = pltpu.VMEM((256, 256), jnp.bfloat16)
    held = pltpu.VMEM(HOME, jnp.float32)
    state = call(first_kernel, "first", HOME, (scalars, state, levels, diagonal_angles[0:1]))
    state = call(second_kernel, "second", AWAY, (scalars, state, swap_core(state)), (table,))
    state = exchange(state.reshape(64, 2, 32, 128)).reshape(AWAY)
    state = call(
        third_kernel, "third", HOME, (scalars, state, away_levels, diagonal_angles[1:2]), (table, held)
    )
    state = call(fourth_kernel, "fourth", AWAY, (scalars, state, swap_core(state)))
    state = exchange(state.reshape(64, 2, 32, 128)).reshape(AWAY)
    state = call(fifth_kernel, "fifth", HOME, (scalars, state), (held,))
    return state.reshape(amplitudes.shape)


def solution(mesh):
    torus = Mesh(mesh.devices.reshape(4, 2, 4, 4), AXES)
    in_specs = (P(None, AXES, None, None), P(AXES, None, None), P(), P())
    out_specs = P(None, AXES, None, None)
    return jax.shard_map(body, mesh=torus, in_specs=in_specs, out_specs=out_specs, check_vma=False)
```

```python
import jax
import jax.numpy as jnp
import numpy as np
from jax import lax
from jax.experimental import pallas as pl
from jax.experimental.pallas import tpu as pltpu
from jax.sharding import Mesh
from jax.sharding import PartitionSpec as P

AXES = ("x", "c", "z", "y")
ORDER = ("y", "z", "x", "c")
VMEM = pltpu.VMEM
SMEM = pltpu.SMEM
PIECES = 4
HOME = (2, 8, 32, 8, 128)
SENT = (8, 16, 3, 2, 8, 128)
AWAY = (8, 16, 2, 2, 8, 128)
ROW, BLOCK, MIDDLE = 0, 1, 2


def fit(fn, terms, most=5.77):
    k = np.arange(400)
    s = most / 2 * (1 + np.cos(np.pi * (k + 0.5) / 400))
    series = np.polynomial.Chebyshev.fit(s, fn(np.sqrt(s)), terms - 1, domain=[0, most])
    return [float(c) for c in series.convert(kind=np.polynomial.Polynomial).coef]


COS = fit(np.cos, 8)
SIN = fit(lambda t: np.sinc(t / np.pi), 7)


def horner(coef, s):
    total = s * coef[-1] + coef[-2]
    for c in coef[-3::-1]:
        total = total * s + c
    return total


def cos_sin(turn):
    square = turn * turn
    return horner(COS, square), horner(SIN, square) * turn


def phase(re, im, level, angle):
    cos, sin = cos_sin(level * angle)
    return re * cos + im * sin, im * cos - re * sin


def rotate(tiles, bit, tan):
    step = 1 << bit
    out = list(tiles)
    for i, u in enumerate(tiles):
        if not i & step:
            v = tiles[i + step]
            out[i] = u - tan * v
            out[i + step] = v + tan * u
    return out


def rotate_all(tiles, tans):
    for bit, tan in zip(reversed(range(len(tans))), tans):
        tiles = rotate(tiles, bit, tan)
    return tiles


def rotate_sublanes(tiles, tan):
    place = lax.broadcasted_iota(jnp.int32, (8, 128), 0)
    for bit in range(3):
        step = 1 << bit
        one = (place & step) != 0
        weight = jnp.where(one, tan, -tan)
        out = []
        for t in tiles:
            other = pltpu.roll(t, step, 0)
            if step < 4:
                other = jnp.where(one, other, pltpu.roll(t, 8 - step, 0))
            out.append(t + weight * other)
        tiles = out
    return tiles


def store_table(turn, layer, table_ref):
    cos, sin = [], []
    for g in range(4):
        c, s = cos_sin(jnp.full((8, 128), turn[layer, g], jnp.float32))
        cos.append(c)
        sin.append(s)
    pair = cos[1] * cos[2]
    cube = pair * pair * pair
    scale = cube * cube * pair * (cos[3] * cos[3]) * (cos[3] * cos[3])
    col = lax.broadcasted_iota(jnp.int32, (8, 128), 1)
    sub = lax.broadcasted_iota(jnp.int32, (8, 128), 0)
    for bit in range(3):
        a, b = (sub >> bit) & 1, (col >> bit) & 1
        scale = scale * jnp.where(a == b, cos[0], jnp.where(b == 1, sin[0], -sin[0]))
    for k in range(16):
        table = scale
        for bit in range(4):
            b = (col >> (bit + 3)) & 1
            if (k >> bit) & 1:
                table = table * jnp.where(b == 1, cos[0], -sin[0])
            else:
                table = table * jnp.where(b == 1, sin[0], cos[0])
        high = table.astype(jnp.bfloat16)
        low = (table - high.astype(jnp.float32)).astype(jnp.bfloat16)
        rows = slice(8 * k, 8 * k + 8)
        more = slice(128 + 8 * k, 136 + 8 * k)
        table_ref[rows, 0:128] = high
        table_ref[rows, 128:256] = low
        table_ref[more, 0:128] = high
        table_ref[more, 128:256] = jnp.zeros_like(high)
    return [sin[g] / cos[g] for g in (1, 2, 3)]


def mix_lanes(tiles, table_ref):
    rows = jnp.concatenate(tiles, axis=0)
    high = rows.astype(jnp.bfloat16)
    low = (rows - high.astype(jnp.float32)).astype(jnp.bfloat16)
    both = jnp.dot(
        jnp.concatenate([high, low], axis=1), table_ref[...], preferred_element_type=jnp.float32
    )
    mixed = both[:, 0:128] + both[:, 128:256]
    return [mixed[8 * i : 8 * i + 8] for i in range(len(tiles))]


def first_kernel(
    turn_hbm, angle_hbm, state_hbm, levels_hbm, out, tans, next_table, turn, angle, state, table, sems
):
    small = [
        pltpu.make_async_copy(turn_hbm, turn, sems.at[0]),
        pltpu.make_async_copy(angle_hbm, angle, sems.at[1]),
    ]
    copies = []
    for k in range(PIECES):
        js, qs = pl.ds(32 // PIECES * k, 32 // PIECES), pl.ds(16 // PIECES * k, 16 // PIECES)
        copies.append(
            (
                pltpu.make_async_copy(levels_hbm.at[:, qs], out.at[:, qs, 2], sems.at[2 + 2 * k]),
                pltpu.make_async_copy(state_hbm.at[:, :, js], state.at[:, :, js], sems.at[3 + 2 * k]),
            )
        )
    for c in small:
        c.start()
    for pair in copies:
        for c in pair:
            c.start()
    for c in small:
        c.wait()
    row0, block0, middle0 = store_table(turn, 0, table)
    later = store_table(turn, 1, next_table)
    for i, t in enumerate([row0, block0, middle0, *later]):
        tans[i] = t
    turned = jnp.broadcast_to(angle[0:1], (8, 128))

    for k in range(PIECES):
        for c in copies[k]:
            c.wait()

        @pl.loop(32 // PIECES * k, 32 // PIECES * (k + 1))
        def _(j):
            re, im = [], []
            for i in range(8):
                level = out[i, j >> 1, 2, j & 1]
                a, b = phase(state[0, i, j], state[1, i, j], level, turned)
                re.append(a)
                im.append(b)
            for p, tiles in enumerate((re, im)):
                tiles = rotate_all(tiles, [block0] * 3)
                for i in range(8):
                    state[p, i, j] = tiles[i]

    @pl.loop(0, 8)
    def _(b):
        for p in range(2):
            tiles = mix_lanes([state[p, b, i] for i in range(32)], table)
            tiles = rotate_all(tiles, [block0, row0, row0, row0, row0])
            tiles = rotate_sublanes(tiles, row0)
            for i in range(32):
                out[b, i >> 1, p, i & 1] = tiles[i]


def second_kernel(state, angle, tans, table, out, held):
    block0, middle0 = tans[BLOCK], tans[MIDDLE]
    row1, block1, middle1 = tans[3 + ROW], tans[3 + BLOCK], tans[3 + MIDDLE]
    turned = jnp.broadcast_to(angle[1:2], (8, 128))

    @pl.loop(0, 32)
    def _(j):
        for p in range(2):
            tiles = rotate_all([state[i, j >> 1, p, j & 1] for i in range(8)], [middle0] * 3)
            for i in range(8):
                held[p, i, j] = tiles[i]

    @pl.loop(0, 8)
    def _(b):
        parts = [[None] * 32, [None] * 32]
        for r in range(2):
            two = []
            for p in range(2):
                tiles = [held[p, b, 2 * q + r] for q in range(16)]
                two.append(rotate_all(tiles, [middle0, block0, block0, block0]))
            for q in range(16):
                re, im = phase(two[0][q], two[1][q], state[b, q, 2, r], turned)
                parts[0][2 * q + r], parts[1][2 * q + r] = re, im
        for p in range(2):
            tiles = mix_lanes(parts[p], table)
            tiles = rotate_all(tiles, [middle1, block1, block1, block1, row1])
            tiles = rotate_sublanes(tiles, row1)
            for i in range(32):
                held[p, b, i] = tiles[i]

    @pl.loop(0, 32)
    def _(j):
        for p in range(2):
            tiles = rotate_all([held[p, i, j] for i in range(8)], [middle1] * 3)
            for i in range(8):
                out[i, j >> 1, p, j & 1] = tiles[i]


def third_kernel(state, tans, out_hbm, held, done, sems):
    row, block = tans[3 + ROW], tans[3 + BLOCK]

    @pl.loop(0, 32)
    def _(j):
        for p in range(2):
            tiles = rotate_all([state[i, j >> 1, p, j & 1] for i in range(8)], [block] * 3)
            for i in range(8):
                held[p, i, j] = tiles[i]

    copies = []
    for b in range(8):
        for p in range(2):
            for r in range(2):
                tiles = rotate_all([held[p, b, 2 * q + r] for q in range(16)], [block, row, row, row])
                for q in range(16):
                    done[p, b, 2 * q + r] = tiles[q]
        copies.append(pltpu.make_async_copy(done.at[:, b], out_hbm.at[:, b], sems.at[b]))
        copies[-1].start()
    for c in copies:
        c.wait()


def spec(space):
    return pl.BlockSpec(memory_space=space)


def call(kernel, name, shapes, ins, outs, inputs, scratch, flops, limit):
    return pl.pallas_call(
        kernel,
        out_shape=[jax.ShapeDtypeStruct(s, d) for s, d in shapes],
        in_specs=[spec(s) for s in ins],
        out_specs=[spec(s) for s in outs],
        scratch_shapes=list(scratch),
        name=name,
        cost_estimate=pl.CostEstimate(flops=flops, bytes_accessed=5 << 20, transcendentals=0),
        compiler_params=pltpu.CompilerParams(vmem_limit_bytes=limit << 20),
    )(*inputs)


def exchange(state, shape):
    flat = lax.all_to_all(state.reshape(128, -1, 128), ORDER, 0, 0, tiled=True)
    return flat.reshape(shape)


def body(amplitudes, energies, diagonal_angles, turn_angles):
    f32, bf16 = jnp.float32, jnp.bfloat16
    table = VMEM((256, 256), bf16)
    state, tans, next_table = call(
        first_kernel,
        "first",
        [(SENT, f32), ((6, 8, 128), f32), ((256, 256), bf16)],
        [pltpu.HBM] * 4,
        [VMEM] * 3,
        (turn_angles, diagonal_angles, amplitudes.reshape(HOME), energies.reshape(8, 16, 2, 8, 128)),
        [
            SMEM((2, 4), f32),
            VMEM((2, 128), f32),
            VMEM(HOME, f32),
            table,
            pltpu.SemaphoreType.DMA((2 + 2 * PIECES,)),
        ],
        20_000_000,
        16,
    )
    state = exchange(state, SENT)
    (state,) = call(
        second_kernel,
        "second",
        [(AWAY, f32)],
        [VMEM] * 4,
        [VMEM],
        (state, diagonal_angles, tans, next_table),
        [VMEM(HOME, f32)],
        20_000_000,
        16,
    )
    state = exchange(state, AWAY)
    (state,) = call(
        third_kernel,
        "third",
        [(HOME, f32)],
        [VMEM] * 2,
        [pltpu.HBM],
        (state, tans),
        [VMEM(HOME, f32), VMEM(HOME, f32), pltpu.SemaphoreType.DMA((8,))],
        10_000_000,
        16,
    )
    return state.reshape(amplitudes.shape)


def solution(mesh):
    torus = Mesh(mesh.devices.reshape(4, 2, 4, 4), AXES)
    in_specs = (P(None, AXES, None, None), P(AXES, None, None), P(), P())
    out_specs = P(None, AXES, None, None)
    return jax.shard_map(body, mesh=torus, in_specs=in_specs, out_specs=out_specs, check_vma=False)
```

```python
import jax
import jax.numpy as jnp
import numpy as np
from jax import lax
from jax.experimental import pallas as pl
from jax.experimental.pallas import tpu as pltpu
from jax.sharding import Mesh
from jax.sharding import PartitionSpec as P

AXES = ("x", "c", "z", "y")
ORDER = ("y", "z", "x", "c")
VMEM = pltpu.VMEM
SMEM = pltpu.SMEM
PIECES = 4
HOME = (2, 8, 32, 8, 128)
SENT = (8, 16, 3, 2, 8, 128)
AWAY = (8, 16, 2, 2, 8, 128)
ROW, BLOCK, MIDDLE = 0, 1, 2


def fit(fn, terms, most=5.77):
    k = np.arange(400)
    s = most / 2 * (1 + np.cos(np.pi * (k + 0.5) / 400))
    series = np.polynomial.Chebyshev.fit(s, fn(np.sqrt(s)), terms - 1, domain=[0, most])
    return [float(c) for c in series.convert(kind=np.polynomial.Polynomial).coef]


COS = fit(lambda t: np.sqrt(2) * np.cos(t / 2), 5)
SIN = fit(lambda t: np.sqrt(0.5) * np.sinc(t / 2 / np.pi), 5)


def horner(coef, s):
    total = s * coef[-1] + coef[-2]
    for c in coef[-3::-1]:
        total = total * s + c
    return total


def cos_sin(turn):
    square = turn * turn
    cos, sin = horner(COS, square), horner(SIN, square) * turn
    return 1.0 - sin * sin, sin * cos


def phase(re, im, level, angle):
    cos, sin = cos_sin(level * angle)
    return re * cos + im * sin, im * cos - re * sin


def rotate(tiles, bit, tan):
    step = 1 << bit
    out = list(tiles)
    for i, u in enumerate(tiles):
        if not i & step:
            v = tiles[i + step]
            out[i] = u - tan * v
            out[i + step] = v + tan * u
    return out


def rotate_all(tiles, tans):
    for bit, tan in zip(reversed(range(len(tans))), tans):
        tiles = rotate(tiles, bit, tan)
    return tiles


def rotate_sublanes(tiles, tan):
    place = lax.broadcasted_iota(jnp.int32, (8, 128), 0)
    for bit in range(3):
        step = 1 << bit
        weight = jnp.where((place & step) != 0, tan, -tan)
        tiles = [t + weight * jnp.take_along_axis(t, place ^ step, axis=0) for t in tiles]
    return tiles


def store_table(turn, layer, table_ref):
    cos, sin = [], []
    for g in range(4):
        c, s = cos_sin(jnp.full((8, 128), turn[layer, g], jnp.float32))
        cos.append(c)
        sin.append(s)
    pair = cos[1] * cos[2]
    cube = pair * pair * pair
    scale = cube * cube * pair * (cos[3] * cos[3]) * (cos[3] * cos[3])
    col = lax.broadcasted_iota(jnp.int32, (8, 128), 1)
    sub = lax.broadcasted_iota(jnp.int32, (8, 128), 0)
    for bit in range(3):
        a, b = (sub >> bit) & 1, (col >> bit) & 1
        scale = scale * jnp.where(a == b, cos[0], jnp.where(b == 1, sin[0], -sin[0]))
    for k in range(16):
        table = scale
        for bit in range(4):
            b = (col >> (bit + 3)) & 1
            if (k >> bit) & 1:
                table = table * jnp.where(b == 1, cos[0], -sin[0])
            else:
                table = table * jnp.where(b == 1, sin[0], cos[0])
        high = table.astype(jnp.bfloat16)
        low = (table - high.astype(jnp.float32)).astype(jnp.bfloat16)
        rows = slice(8 * k, 8 * k + 8)
        more = slice(128 + 8 * k, 136 + 8 * k)
        table_ref[rows, 0:128] = high
        table_ref[rows, 128:256] = low
        table_ref[more, 0:128] = high
        table_ref[more, 128:256] = jnp.zeros_like(high)
    return [sin[g] / cos[g] for g in (1, 2, 3)]


def mix_lanes(tiles, table_ref):
    rows = jnp.concatenate(tiles, axis=0)
    high = rows.astype(jnp.bfloat16)
    low = (rows - high.astype(jnp.float32)).astype(jnp.bfloat16)
    both = jnp.dot(
        jnp.concatenate([high, low], axis=1), table_ref[...], preferred_element_type=jnp.float32
    )
    mixed = both[:, 0:128] + both[:, 128:256]
    return [mixed[8 * i : 8 * i + 8] for i in range(len(tiles))]


def first_kernel(
    turn_hbm, angle_hbm, state_hbm, levels_hbm, out, tans, next_table, turn, angle, state, table, sems
):
    small = [
        pltpu.make_async_copy(turn_hbm, turn, sems.at[0]),
        pltpu.make_async_copy(angle_hbm, angle, sems.at[1]),
    ]
    copies = []
    for k in range(PIECES):
        js, qs = pl.ds(32 // PIECES * k, 32 // PIECES), pl.ds(16 // PIECES * k, 16 // PIECES)
        copies.append(
            (
                pltpu.make_async_copy(levels_hbm.at[:, qs], out.at[:, qs, 2], sems.at[2 + 2 * k]),
                pltpu.make_async_copy(state_hbm.at[:, :, js], state.at[:, :, js], sems.at[3 + 2 * k]),
            )
        )
    for c in small:
        c.start()
    for pair in copies:
        for c in pair:
            c.start()
    for c in small:
        c.wait()
    row0, block0, middle0 = store_table(turn, 0, table)
    later = store_table(turn, 1, next_table)
    for i, t in enumerate([row0, block0, middle0, *later]):
        tans[i] = t
    turned = jnp.broadcast_to(angle[0:1], (8, 128))

    for k in range(PIECES):
        for c in copies[k]:
            c.wait()

        @pl.loop(32 // PIECES * k, 32 // PIECES * (k + 1))
        def _(j):
            re, im = [], []
            for i in range(8):
                level = out[i, j >> 1, 2, j & 1]
                a, b = phase(state[0, i, j], state[1, i, j], level, turned)
                re.append(a)
                im.append(b)
            for p, tiles in enumerate((re, im)):
                tiles = rotate_all(tiles, [block0] * 3)
                for i in range(8):
                    state[p, i, j] = tiles[i]

    @pl.loop(0, 8)
    def _(b):
        for p in range(2):
            tiles = mix_lanes([state[p, b, i] for i in range(32)], table)
            tiles = rotate_all(tiles, [block0, row0, row0, row0, row0])
            tiles = rotate_sublanes(tiles, row0)
            for i in range(32):
                out[b, i >> 1, p, i & 1] = tiles[i]


def second_kernel(state, angle, tans, table, out, held):
    block0, middle0 = tans[BLOCK], tans[MIDDLE]
    row1, block1, middle1 = tans[3 + ROW], tans[3 + BLOCK], tans[3 + MIDDLE]
    turned = jnp.broadcast_to(angle[1:2], (8, 128))

    @pl.loop(0, 32)
    def _(j):
        for p in range(2):
            tiles = rotate_all([state[i, j >> 1, p, j & 1] for i in range(8)], [middle0] * 3)
            for i in range(8):
                held[p, i, j] = tiles[i]

    @pl.loop(0, 8)
    def _(b):
        parts = [[None] * 32, [None] * 32]
        for r in range(2):
            two = []
            for p in range(2):
                tiles = [held[p, b, 2 * q + r] for q in range(16)]
                two.append(rotate_all(tiles, [middle0, block0, block0, block0]))
            for q in range(16):
                re, im = phase(two[0][q], two[1][q], state[b, q, 2, r], turned)
                parts[0][2 * q + r], parts[1][2 * q + r] = re, im
        for p in range(2):
            tiles = mix_lanes(parts[p], table)
            tiles = rotate_all(tiles, [middle1, block1, block1, block1, row1])
            tiles = rotate_sublanes(tiles, row1)
            for i in range(32):
                held[p, b, i] = tiles[i]

    @pl.loop(0, 32)
    def _(j):
        for p in range(2):
            tiles = rotate_all([held[p, i, j] for i in range(8)], [middle1] * 3)
            for i in range(8):
                out[i, j >> 1, p, j & 1] = tiles[i]


def third_kernel(state, tans, out_hbm, held, done, sems):
    row, block = tans[3 + ROW], tans[3 + BLOCK]

    @pl.loop(0, 32)
    def _(j):
        for p in range(2):
            tiles = rotate_all([state[i, j >> 1, p, j & 1] for i in range(8)], [block] * 3)
            for i in range(8):
                held[p, i, j] = tiles[i]

    copies = []
    for b in range(8):
        for p in range(2):
            for r in range(2):
                tiles = rotate_all([held[p, b, 2 * q + r] for q in range(16)], [block, row, row, row])
                for q in range(16):
                    done[p, b, 2 * q + r] = tiles[q]
        copies.append(pltpu.make_async_copy(done.at[:, b], out_hbm.at[:, b], sems.at[b]))
        copies[-1].start()
    for c in copies:
        c.wait()


def spec(space):
    return pl.BlockSpec(memory_space=space)


def call(kernel, name, shapes, ins, outs, inputs, scratch, flops, limit):
    return pl.pallas_call(
        kernel,
        out_shape=[jax.ShapeDtypeStruct(s, d) for s, d in shapes],
        in_specs=[spec(s) for s in ins],
        out_specs=[spec(s) for s in outs],
        scratch_shapes=list(scratch),
        name=name,
        cost_estimate=pl.CostEstimate(flops=flops, bytes_accessed=5 << 20, transcendentals=0),
        compiler_params=pltpu.CompilerParams(vmem_limit_bytes=limit << 20),
    )(*inputs)


def exchange(state, shape):
    flat = lax.all_to_all(state.reshape(128, -1, 128), ORDER, 0, 0, tiled=True)
    return flat.reshape(shape)


def body(amplitudes, energies, diagonal_angles, turn_angles):
    f32, bf16 = jnp.float32, jnp.bfloat16
    table = VMEM((256, 256), bf16)
    state, tans, next_table = call(
        first_kernel,
        "first",
        [(SENT, f32), ((6, 8, 128), f32), ((256, 256), bf16)],
        [pltpu.HBM] * 4,
        [VMEM] * 3,
        [
            pltpu.with_memory_space_constraint(a, pltpu.HBM)
            for a in (
                turn_angles,
                diagonal_angles,
                amplitudes.reshape(HOME),
                energies.reshape(8, 16, 2, 8, 128),
            )
        ],
        [
            SMEM((2, 4), f32),
            VMEM((2, 128), f32),
            VMEM(HOME, f32),
            table,
            pltpu.SemaphoreType.DMA((2 + 2 * PIECES,)),
        ],
        20_000_000,
        16,
    )
    state = exchange(state, SENT)
    (state,) = call(
        second_kernel,
        "second",
        [(AWAY, f32)],
        [VMEM] * 4,
        [VMEM],
        (state, diagonal_angles, tans, next_table),
        [VMEM(HOME, f32)],
        20_000_000,
        16,
    )
    state = exchange(state, AWAY)
    (state,) = call(
        third_kernel,
        "third",
        [(HOME, f32)],
        [VMEM] * 2,
        [pltpu.HBM],
        (state, tans),
        [VMEM(HOME, f32), VMEM(HOME, f32), pltpu.SemaphoreType.DMA((8,))],
        10_000_000,
        16,
    )
    return state.reshape(amplitudes.shape)


def solution(mesh):
    torus = Mesh(mesh.devices.reshape(4, 2, 4, 4), AXES)
    in_specs = (P(None, AXES, None, None), P(AXES, None, None), P(), P())
    out_specs = P(None, AXES, None, None)
    return jax.shard_map(body, mesh=torus, in_specs=in_specs, out_specs=out_specs, check_vma=False)
```

```python
import jax
import jax.numpy as jnp
import numpy as np
from jax import lax
from jax.experimental import pallas as pl
from jax.experimental.pallas import tpu as pltpu
from jax.sharding import Mesh
from jax.sharding import PartitionSpec as P

AXES = ("x", "c", "z", "y")
ORDER = ("y", "z", "x", "c")
VMEM = pltpu.VMEM
SMEM = pltpu.SMEM
AHEAD = 4
HOME = (2, 8, 32, 8, 128)
SENT = (8, 16, 3, 2, 8, 128)
AWAY = (8, 16, 2, 2, 8, 128)
LANES, ROWS, BLOCK, MIDDLE = range(4)


def fit(fn, terms, most=5.77):
    k = np.arange(400)
    s = most / 2 * (1 + np.cos(np.pi * (k + 0.5) / 400))
    series = np.polynomial.Chebyshev.fit(s, fn(np.sqrt(s)), terms - 1, domain=[0, most])
    return [float(c) for c in series.convert(kind=np.polynomial.Polynomial).coef]


COS = fit(lambda t: np.sqrt(2) * np.cos(t / 2), 5)
SIN = fit(lambda t: np.sqrt(0.5) * np.sinc(t / 2 / np.pi), 5)


def horner(coef, s):
    total = s * coef[-1] + coef[-2]
    for c in coef[-3::-1]:
        total = total * s + c
    return total


def cos_sin(turn):
    square = turn * turn
    cos, sin = horner(COS, square), horner(SIN, square) * turn
    return 1.0 - sin * sin, sin * cos


def phase(re, im, level, angle):
    cos, sin = cos_sin(level * angle)
    return re * cos + im * sin, im * cos - re * sin


def rotate(tiles, bit, tan):
    step = 1 << bit
    out = list(tiles)
    for i, u in enumerate(tiles):
        if not i & step:
            v = tiles[i + step]
            out[i] = u - tan * v
            out[i + step] = v + tan * u
    return out


def rotate_all(tiles, tans):
    for bit, tan in zip(reversed(range(len(tans))), tans):
        tiles = rotate(tiles, bit, tan)
    return tiles


def kron(columns, pairs):
    tiles = [columns]
    for zero, one in pairs:
        tiles = [t * f for t in tiles for f in (zero, one)]
    return tiles


def split(values):
    high = values.astype(jnp.bfloat16)
    return high, (values - high.astype(jnp.float32)).astype(jnp.bfloat16)


def turn_factors(turn, layer):
    pairs = [cos_sin(jnp.full((8, 128), turn[layer, g], jnp.float32)) for g in range(4)]
    return [c for c, _ in pairs], [s for _, s in pairs]


def store_tables(cos, sin, rest, bits, lanes_ref, rows_ref):
    col = lax.broadcasted_iota(jnp.int32, (8, 128), 1)
    sub = lax.broadcasted_iota(jnp.int32, (8, 128), 0)

    def pair(bit, cos, sin, back):
        one = ((col >> bit) & 1) == 1
        if back:
            return jnp.where(one, -sin, cos), jnp.where(one, cos, sin)
        return jnp.where(one, sin, cos), jnp.where(one, cos, -sin)

    def low(cos, sin, back):
        table = jnp.ones((8, 128), jnp.float32)
        for bit in range(3):
            zero, one = pair(bit, cos, sin, back)
            table = table * jnp.where(((sub >> bit) & 1) == 1, one, zero)
        return table

    tiles = kron(low(cos[0], sin[0], False) * rest, [pair(k, cos[0], sin[0], False) for k in (6, 5, 4, 3)])
    for k, t in enumerate(tiles):
        high, less = split(t)
        rows, more = slice(8 * k, 8 * k + 8), slice(128 + 8 * k, 136 + 8 * k)
        lanes_ref[rows, 0:128] = high
        lanes_ref[rows, 128:256] = less
        lanes_ref[more, 0:128] = high
        lanes_ref[more, 128:256] = jnp.zeros_like(high)
    tiles = low(cos[ROWS], sin[ROWS], True)
    g = bits[0]
    for half, top in enumerate(((cos[g], sin[g]), (-sin[g], cos[g]))):
        pairs = [pair(6 - k, cos[h], sin[h], True) for k, h in enumerate(bits[1:])]
        for k, t in enumerate(kron(tiles, [top] + pairs)):
            high, less = split(t)
            rows = slice(8 * k, 8 * k + 8)
            for third, part in enumerate((high, high, less)):
                at = 256 * third + 128 * half
                rows_ref[rows, at : at + 128] = part


def mix(parts, lanes_ref, rows_ref):
    highs, lows = [], []
    for tiles in parts:
        both = jnp.dot(
            jnp.concatenate(split(jnp.concatenate(tiles, axis=0)), axis=1),
            lanes_ref[...],
            preferred_element_type=jnp.float32,
        )
        high, low = split(both[:, 0:128] + both[:, 128:256])
        highs.append(high)
        lows.append(low)
    high, low = jnp.concatenate(highs, axis=1), jnp.concatenate(lows, axis=1)
    mixed = jnp.dot(
        rows_ref[...], jnp.concatenate([high, low, high], axis=0), preferred_element_type=jnp.float32
    )
    return [[mixed[8 * i : 8 * i + 8, 128 * p : 128 * p + 128] for i in range(32)] for p in range(2)]


def in_step(prepare, finish, blocks):
    for k in range(5):
        now, last = blocks[k % 2], blocks[(k + 1) % 2]
        if k < 4:
            prepare(2 * k, now, 0)
            prepare(2 * k + 1, now, 1)
        if k:
            finish(2 * k - 2, last, 0)
            finish(2 * k - 1, last, 1)


def mix_block(block, at, lanes, rows, held, b):
    parts = mix([[block[at, p, i] for i in range(32)] for p in range(2)], lanes, rows)
    for p in range(2):
        for i in range(32):
            held[p, b, i] = parts[p][i]


def first_kernel(
    turn_hbm,
    angle_hbm,
    state_hbm,
    levels_hbm,
    out,
    tans,
    next_lanes,
    next_rows,
    turn,
    angle,
    state,
    lanes,
    rows,
    even,
    odd,
    sems,
):
    small = [
        pltpu.make_async_copy(turn_hbm, turn, sems.at[0]),
        pltpu.make_async_copy(angle_hbm, angle, sems.at[1]),
    ]
    copies = [
        (
            pltpu.make_async_copy(levels_hbm.at[b], out.at[b, :, 2], sems.at[2 + 2 * b]),
            pltpu.make_async_copy(state_hbm.at[:, b], state.at[:, b], sems.at[3 + 2 * b]),
        )
        for b in range(8)
    ]

    def start(b):
        for c in copies[b]:
            c.start()

    for c in small:
        c.start()
    for b in range(AHEAD):
        start(b)
    for c in small:
        c.wait()
    cos, sin = turn_factors(turn, 0)
    for g in range(1, 4):
        tans[g] = sin[g] / cos[g]
    block0 = tans[BLOCK]
    two, four = cos[BLOCK] * cos[BLOCK], cos[MIDDLE] * cos[MIDDLE]
    rest = two * two * two * four * four
    store_tables(cos, sin, rest, (BLOCK, ROWS, ROWS, ROWS, ROWS), lanes, rows)
    cos, sin = turn_factors(turn, 1)
    for g in range(1, 4):
        tans[4 + g] = sin[g] / cos[g]
    pair = cos[ROWS] * cos[BLOCK] * cos[MIDDLE]
    rest = pair * pair * pair * cos[BLOCK]
    store_tables(cos, sin, rest, (MIDDLE, BLOCK, BLOCK, BLOCK, ROWS), next_lanes, next_rows)
    turned = jnp.broadcast_to(angle[0:1], (8, 128))

    def prepare(b, block, at):
        if not at:
            for k in (b, b + 1):
                for c in copies[k]:
                    c.wait()
                if k + AHEAD < 8:
                    start(k + AHEAD)
        for i in range(32):
            level = out[b, i >> 1, 2, i & 1]
            block[at, 0, i], block[at, 1, i] = phase(state[0, b, i], state[1, b, i], level, turned)

    def finish(b, block, at):
        mix_block(block, at, lanes, rows, state, b)

    in_step(prepare, finish, (even, odd))

    @pl.loop(0, 32, unroll=4)
    def _(j):
        for p in range(2):
            tiles = rotate_all([state[p, i, j] for i in range(8)], [block0] * 3)
            for i in range(8):
                out[i, j >> 1, p, j & 1] = tiles[i]


def second_kernel(state, angle, tans, lanes, rows, out, held, even, odd):
    block0, middle0, middle1 = tans[BLOCK], tans[MIDDLE], tans[4 + MIDDLE]
    turned = jnp.broadcast_to(angle[1:2], (8, 128))

    @pl.loop(0, 32, unroll=4)
    def _(j):
        for p in range(2):
            tiles = rotate_all([state[i, j >> 1, p, j & 1] for i in range(8)], [middle0] * 3)
            for i in range(8):
                held[p, i, j] = tiles[i]

    def prepare(b, block, at):
        for r in range(2):
            re, im = (
                rotate_all([held[p, b, 2 * q + r] for q in range(16)], [middle0, block0, block0, block0])
                for p in range(2)
            )
            for q in range(16):
                level = state[b, q, 2, r]
                i = 2 * q + r
                block[at, 0, i], block[at, 1, i] = phase(re[q], im[q], level, turned)

    def finish(b, block, at):
        mix_block(block, at, lanes, rows, held, b)

    in_step(prepare, finish, (even, odd))

    @pl.loop(0, 32, unroll=4)
    def _(j):
        for p in range(2):
            tiles = rotate_all([held[p, i, j] for i in range(8)], [middle1] * 3)
            for i in range(8):
                out[i, j >> 1, p, j & 1] = tiles[i]


def third_kernel(state, tans, out_hbm, held, done, sems):
    row, block = tans[4 + ROWS], tans[4 + BLOCK]

    @pl.loop(0, 32, unroll=4)
    def _(j):
        for p in range(2):
            tiles = rotate_all([state[i, j >> 1, p, j & 1] for i in range(8)], [block] * 3)
            for i in range(8):
                held[p, i, j] = tiles[i]

    copies = []
    for b in range(8):
        for p in range(2):
            for r in range(2):
                tiles = rotate_all([held[p, b, 2 * q + r] for q in range(16)], [block, row, row, row])
                for q in range(16):
                    done[p, b, 2 * q + r] = tiles[q]
        copies.append(pltpu.make_async_copy(done.at[:, b], out_hbm.at[:, b], sems.at[b]))
        copies[-1].start()
    for c in copies:
        c.wait()


def spec(space):
    return pl.BlockSpec(memory_space=space)


def call(kernel, name, shapes, ins, outs, inputs, scratch, flops, limit):
    return pl.pallas_call(
        kernel,
        out_shape=[jax.ShapeDtypeStruct(s, d) for s, d in shapes],
        in_specs=[spec(s) for s in ins],
        out_specs=[spec(s) for s in outs],
        scratch_shapes=list(scratch),
        name=name,
        cost_estimate=pl.CostEstimate(flops=flops, bytes_accessed=5 << 20, transcendentals=0),
        compiler_params=pltpu.CompilerParams(vmem_limit_bytes=limit << 20),
    )(*inputs)


def exchange(state, shape):
    flat = lax.all_to_all(state.reshape(128, -1, 128), ORDER, 0, 0, tiled=True)
    return flat.reshape(shape)


def body(amplitudes, energies, diagonal_angles, turn_angles):
    f32, bf16 = jnp.float32, jnp.bfloat16
    block = VMEM((2, 2, 32, 8, 128), f32)
    state, tans, lanes, rows = call(
        first_kernel,
        "first",
        [(SENT, f32), ((8, 8, 128), f32), ((256, 256), bf16), ((256, 768), bf16)],
        [pltpu.HBM] * 4,
        [VMEM] * 4,
        [
            pltpu.with_memory_space_constraint(a, pltpu.HBM)
            for a in (
                turn_angles,
                diagonal_angles,
                amplitudes.reshape(HOME),
                energies.reshape(8, 16, 2, 8, 128),
            )
        ],
        [
            SMEM((2, 4), f32),
            VMEM((2, 128), f32),
            VMEM(HOME, f32),
            VMEM((256, 256), bf16),
            VMEM((256, 768), bf16),
            block,
            block,
            pltpu.SemaphoreType.DMA((18,)),
        ],
        20_000_000,
        16,
    )
    state = exchange(state, SENT)
    (state,) = call(
        second_kernel,
        "second",
        [(AWAY, f32)],
        [VMEM] * 5,
        [VMEM],
        (state, diagonal_angles, tans, lanes, rows),
        [VMEM(HOME, f32), block, block],
        20_000_000,
        16,
    )
    state = exchange(state, AWAY)
    (state,) = call(
        third_kernel,
        "third",
        [(HOME, f32)],
        [VMEM] * 2,
        [pltpu.HBM],
        (state, tans),
        [VMEM(HOME, f32), VMEM(HOME, f32), pltpu.SemaphoreType.DMA((8,))],
        10_000_000,
        16,
    )
    return state.reshape(amplitudes.shape)


def solution(mesh):
    torus = Mesh(mesh.devices.reshape(4, 2, 4, 4), AXES)
    in_specs = (P(None, AXES, None, None), P(AXES, None, None), P(), P())
    out_specs = P(None, AXES, None, None)
    return jax.shard_map(body, mesh=torus, in_specs=in_specs, out_specs=out_specs, check_vma=False)
```

```python
import jax
import jax.numpy as jnp
import numpy as np
from jax import lax
from jax.experimental import pallas as pl
from jax.experimental.pallas import tpu as pltpu
from jax.sharding import Mesh
from jax.sharding import PartitionSpec as P

AXES = ("x", "c", "z", "y")
ORDER = ("y", "z", "x", "c")
VMEM = pltpu.VMEM
SMEM = pltpu.SMEM
HOME = (2, 8, 32, 8, 128)
SENT = (8, 16, 3, 2, 8, 128)
AWAY = (8, 16, 2, 2, 8, 128)
LANES, ROWS, BLOCK, MIDDLE = range(4)


def fit(fn, terms, most=5.77):
    k = np.arange(400)
    s = most / 2 * (1 + np.cos(np.pi * (k + 0.5) / 400))
    series = np.polynomial.Chebyshev.fit(s, fn(np.sqrt(s)), terms - 1, domain=[0, most])
    return [float(c) for c in series.convert(kind=np.polynomial.Polynomial).coef]


SIN = fit(lambda t: np.sqrt(0.5) * np.sinc(t / 2 / np.pi), 4)


def horner(coef, s):
    total = s * coef[-1] + coef[-2]
    for c in coef[-3::-1]:
        total = total * s + c
    return total


def cos_sin(turn):
    half = horner(SIN, turn * turn) * turn
    cos = 1.0 - half * half
    above = 1.0 + cos
    return cos, half * above * lax.rsqrt(above)


def phase(re, im, level, angle):
    cos, sin = cos_sin(level * angle)
    return re * cos + im * sin, im * cos - re * sin


def rotate(tiles, bit, tan):
    step = 1 << bit
    out = list(tiles)
    for i, u in enumerate(tiles):
        if not i & step:
            v = tiles[i + step]
            out[i] = u - tan * v
            out[i + step] = v + tan * u
    return out


def rotate_all(tiles, tans):
    for bit, tan in zip(reversed(range(len(tans))), tans):
        tiles = rotate(tiles, bit, tan)
    return tiles


def kron(columns, pairs):
    tiles = [columns]
    for zero, one in pairs:
        tiles = [t * f for t in tiles for f in (zero, one)]
    return tiles


def split(values):
    high = values.astype(jnp.bfloat16)
    return high, (values - high.astype(jnp.float32)).astype(jnp.bfloat16)


def turn_factors(turn, layer):
    pairs = [cos_sin(jnp.full((8, 128), turn[layer, g], jnp.float32)) for g in range(4)]
    return [c for c, _ in pairs], [s for _, s in pairs]


def store_tables(cos, sin, rest, bits, lanes_ref, rows_ref):
    col = lax.broadcasted_iota(jnp.int32, (8, 128), 1)
    sub = lax.broadcasted_iota(jnp.int32, (8, 128), 0)

    def pair(bit, cos, sin, back):
        one = ((col >> bit) & 1) == 1
        if back:
            return jnp.where(one, -sin, cos), jnp.where(one, cos, sin)
        return jnp.where(one, sin, cos), jnp.where(one, cos, -sin)

    def low(cos, sin, back):
        table = jnp.ones((8, 128), jnp.float32)
        for bit in range(3):
            zero, one = pair(bit, cos, sin, back)
            table = table * jnp.where(((sub >> bit) & 1) == 1, one, zero)
        return table

    tiles = kron(low(cos[0], sin[0], False) * rest, [pair(k, cos[0], sin[0], False) for k in (6, 5, 4, 3)])
    for k, t in enumerate(tiles):
        high, less = split(t)
        rows, more = slice(8 * k, 8 * k + 8), slice(128 + 8 * k, 136 + 8 * k)
        lanes_ref[rows, 0:128] = high
        lanes_ref[rows, 128:256] = less
        lanes_ref[more, 0:128] = high
        lanes_ref[more, 128:256] = jnp.zeros_like(high)
    tiles = low(cos[ROWS], sin[ROWS], True)
    g = bits[0]
    for half, top in enumerate(((cos[g], sin[g]), (-sin[g], cos[g]))):
        pairs = [pair(6 - k, cos[h], sin[h], True) for k, h in enumerate(bits[1:])]
        for k, t in enumerate(kron(tiles, [top] + pairs)):
            high, less = split(t)
            rows = slice(8 * k, 8 * k + 8)
            for third, part in enumerate((high, high, less)):
                at = 256 * third + 128 * half
                rows_ref[rows, at : at + 128] = part


def mix(parts, lanes_ref, rows_ref):
    rows = jnp.concatenate([t for tiles in parts for t in tiles], axis=0)
    both = jnp.dot(
        jnp.concatenate(split(rows), axis=1), lanes_ref[...], preferred_element_type=jnp.float32
    )
    high, low = split(both[:, 0:128] + both[:, 128:256])
    out = []
    for b in range(0, 256 * len(parts), 512):
        h, l = (jnp.concatenate([v[b : b + 256], v[b + 256 : b + 512]], axis=1) for v in (high, low))
        mixed = jnp.dot(
            rows_ref[...], jnp.concatenate([h, l, h], axis=0), preferred_element_type=jnp.float32
        )
        out += [[mixed[8 * i : 8 * i + 8, 128 * p : 128 * p + 128] for i in range(32)] for p in range(2)]
    return out


def in_step(prepare, finish, blocks):
    for k in range(5):
        now, last = blocks[k % 2], blocks[(k + 1) % 2]
        if k < 4:
            prepare(2 * k, now, 0)
            prepare(2 * k + 1, now, 1)
        if k:
            finish(2 * k - 2, last)


def mix_blocks(block, lanes, rows, held, b):
    parts = mix(
        [[block[at, p, i] for i in range(32)] for at in range(2) for p in range(2)], lanes, rows
    )
    for k, tiles in enumerate(parts):
        for i in range(32):
            held[k % 2, b + k // 2, i] = tiles[i]


def first_kernel(
    turn_hbm,
    angle_hbm,
    state_hbm,
    levels_hbm,
    out,
    tans,
    next_lanes,
    next_rows,
    turn,
    angle,
    state,
    lanes,
    rows,
    even,
    odd,
    sems,
):
    small = [
        pltpu.make_async_copy(turn_hbm, turn, sems.at[0]),
        pltpu.make_async_copy(angle_hbm, angle, sems.at[1]),
    ]
    copies = [
        (
            pltpu.make_async_copy(levels_hbm.at[b], out.at[b, :, 2], sems.at[2 + 2 * b]),
            pltpu.make_async_copy(state_hbm.at[:, b], state.at[:, b], sems.at[3 + 2 * b]),
        )
        for b in range(8)
    ]

    for c in small:
        c.start()
    for pair in copies:
        for c in pair:
            c.start()
    for c in small:
        c.wait()
    cos, sin = turn_factors(turn, 0)
    for g in range(1, 4):
        tans[g] = sin[g] / cos[g]
    block0 = tans[BLOCK]
    two, four = cos[BLOCK] * cos[BLOCK], cos[MIDDLE] * cos[MIDDLE]
    rest = two * two * two * four * four
    store_tables(cos, sin, rest, (BLOCK, ROWS, ROWS, ROWS, ROWS), lanes, rows)
    turned = jnp.broadcast_to(angle[0:1], (8, 128))

    def later_tables():
        cos, sin = turn_factors(turn, 1)
        for g in range(1, 4):
            tans[4 + g] = sin[g] / cos[g]
        pair = cos[ROWS] * cos[BLOCK] * cos[MIDDLE]
        rest = pair * pair * pair * cos[BLOCK]
        store_tables(cos, sin, rest, (MIDDLE, BLOCK, BLOCK, BLOCK, ROWS), next_lanes, next_rows)

    def prepare(b, block, at):
        if not at:
            for pair in copies[b : b + 2] if b < 2 else copies[2:] if b == 2 else ():
                for c in pair:
                    c.wait()
            if b == 4:
                later_tables()
        for i in range(32):
            level = out[b, i >> 1, 2, i & 1]
            block[at, 0, i], block[at, 1, i] = phase(state[0, b, i], state[1, b, i], level, turned)

    def finish(b, block):
        mix_blocks(block, lanes, rows, state, b)

    in_step(prepare, finish, (even, odd))

    @pl.loop(0, 32, unroll=4)
    def _(j):
        for p in range(2):
            tiles = rotate_all([state[p, i, j] for i in range(8)], [block0] * 3)
            for i in range(8):
                out[i, j >> 1, p, j & 1] = tiles[i]


def second_kernel(state, angle, tans, lanes, rows, out, held, even, odd):
    block0, middle0, middle1 = tans[BLOCK], tans[MIDDLE], tans[4 + MIDDLE]
    turned = jnp.broadcast_to(angle[1:2], (8, 128))

    @pl.loop(0, 32, unroll=4)
    def _(j):
        for p in range(2):
            tiles = rotate_all([state[i, j >> 1, p, j & 1] for i in range(8)], [middle0] * 3)
            for i in range(8):
                held[p, i, j] = tiles[i]

    def prepare(b, block, at):
        for r in range(2):
            re, im = (
                rotate_all([held[p, b, 2 * q + r] for q in range(16)], [middle0, block0, block0, block0])
                for p in range(2)
            )
            for q in range(16):
                level = state[b, q, 2, r]
                i = 2 * q + r
                block[at, 0, i], block[at, 1, i] = phase(re[q], im[q], level, turned)

    def finish(b, block):
        mix_blocks(block, lanes, rows, held, b)

    in_step(prepare, finish, (even, odd))

    @pl.loop(0, 32, unroll=4)
    def _(j):
        for p in range(2):
            tiles = rotate_all([held[p, i, j] for i in range(8)], [middle1] * 3)
            for i in range(8):
                out[i, j >> 1, p, j & 1] = tiles[i]


def third_kernel(state, tans, out_hbm, held, done, sems):
    row, block = tans[4 + ROWS], tans[4 + BLOCK]
    copies = []
    for p in range(2):

        @pl.loop(0, 32, unroll=4)
        def _(j):
            tiles = rotate_all([state[i, j >> 1, p, j & 1] for i in range(8)], [block] * 3)
            for i in range(8):
                held[p, i, j] = tiles[i]

        for b in range(8):
            for r in range(2):
                tiles = rotate_all([held[p, b, 2 * q + r] for q in range(16)], [block, row, row, row])
                for q in range(16):
                    done[p, b, 2 * q + r] = tiles[q]
            copies.append(pltpu.make_async_copy(done.at[p, b], out_hbm.at[p, b], sems.at[8 * p + b]))
            copies[-1].start()
    for c in copies:
        c.wait()


def spec(space):
    return pl.BlockSpec(memory_space=space)


def call(kernel, name, shapes, ins, outs, inputs, scratch, flops, limit):
    return pl.pallas_call(
        kernel,
        out_shape=[jax.ShapeDtypeStruct(s, d) for s, d in shapes],
        in_specs=[spec(s) for s in ins],
        out_specs=[spec(s) for s in outs],
        scratch_shapes=list(scratch),
        name=name,
        cost_estimate=pl.CostEstimate(flops=flops, bytes_accessed=5 << 20, transcendentals=0),
        compiler_params=pltpu.CompilerParams(vmem_limit_bytes=limit << 20),
    )(*inputs)


def exchange(state, shape):
    flat = lax.all_to_all(state.reshape(128, -1, 128), ORDER, 0, 0, tiled=True)
    return flat.reshape(shape)


def body(amplitudes, energies, diagonal_angles, turn_angles):
    f32, bf16 = jnp.float32, jnp.bfloat16
    block = VMEM((2, 2, 32, 8, 128), f32)
    state, tans, lanes, rows = call(
        first_kernel,
        "first",
        [(SENT, f32), ((8, 8, 128), f32), ((256, 256), bf16), ((256, 768), bf16)],
        [pltpu.HBM] * 4,
        [VMEM] * 4,
        [
            pltpu.with_memory_space_constraint(a, pltpu.HBM)
            for a in (
                turn_angles,
                diagonal_angles,
                amplitudes.reshape(HOME),
                energies.reshape(8, 16, 2, 8, 128),
            )
        ],
        [
            SMEM((2, 4), f32),
            VMEM((2, 128), f32),
            VMEM(HOME, f32),
            VMEM((256, 256), bf16),
            VMEM((256, 768), bf16),
            block,
            block,
            pltpu.SemaphoreType.DMA((18,)),
        ],
        20_000_000,
        16,
    )
    state = exchange(state, SENT)
    (state,) = call(
        second_kernel,
        "second",
        [(AWAY, f32)],
        [VMEM] * 5,
        [VMEM],
        (state, diagonal_angles, tans, lanes, rows),
        [VMEM(HOME, f32), block, block],
        20_000_000,
        16,
    )
    state = exchange(state, AWAY)
    (state,) = call(
        third_kernel,
        "third",
        [(HOME, f32)],
        [VMEM] * 2,
        [pltpu.HBM],
        (state, tans),
        [VMEM(HOME, f32), VMEM(HOME, f32), pltpu.SemaphoreType.DMA((16,))],
        10_000_000,
        16,
    )
    return state.reshape(amplitudes.shape)


def solution(mesh):
    torus = Mesh(mesh.devices.reshape(4, 2, 4, 4), AXES)
    in_specs = (P(None, AXES, None, None), P(AXES, None, None), P(), P())
    out_specs = P(None, AXES, None, None)
    return jax.shard_map(body, mesh=torus, in_specs=in_specs, out_specs=out_specs, check_vma=False)
```

```python
import jax
import jax.numpy as jnp
import numpy as np
from jax import lax
from jax.experimental import pallas as pl
from jax.experimental.pallas import tpu as pltpu
from jax.sharding import Mesh
from jax.sharding import PartitionSpec as P

AXES = ("x", "c", "z", "y")
ORDER = ("z", "y", "x", "c")
VMEM = pltpu.VMEM
SMEM = pltpu.SMEM
HOME = (2, 8, 32, 8, 128)
SENT = (8, 16, 3, 2, 8, 128)
AWAY = (8, 16, 2, 2, 8, 128)
LANES, ROWS, BLOCK, MIDDLE = range(4)
PLACE = [g for a in ORDER for g in {"x": [BLOCK] * 2, "c": [BLOCK], "y": [MIDDLE] * 2, "z": [MIDDLE] * 2}[a]]


def fit(fn, terms, most=5.77):
    k = np.arange(400)
    s = most / 2 * (1 + np.cos(np.pi * (k + 0.5) / 400))
    series = np.polynomial.Chebyshev.fit(s, fn(np.sqrt(s)), terms - 1, domain=[0, most])
    return [float(c) for c in series.convert(kind=np.polynomial.Polynomial).coef]


SIN = fit(lambda t: np.sqrt(0.5) * np.sinc(t / 2 / np.pi), 4)


def horner(coef, s):
    total = s * coef[-1] + coef[-2]
    for c in coef[-3::-1]:
        total = total * s + c
    return total


def cos_sin(turn):
    half = horner(SIN, turn * turn) * turn
    cos = 1.0 - half * half
    above = 1.0 + cos
    return cos, half * above * lax.rsqrt(above)


def phase(re, im, level, angle):
    cos, sin = cos_sin(level * angle)
    return re * cos + im * sin, im * cos - re * sin


def rotate(tiles, bit, tan):
    step = 1 << bit
    out = list(tiles)
    for i, u in enumerate(tiles):
        if not i & step:
            v = tiles[i + step]
            out[i] = u - tan * v
            out[i + step] = v + tan * u
    return out


def rotate_all(tiles, tans):
    for bit, tan in zip(reversed(range(len(tans))), tans):
        tiles = rotate(tiles, bit, tan)
    return tiles


def kron(columns, pairs):
    tiles = [columns]
    for zero, one in pairs:
        tiles = [t * f for t in tiles for f in (zero, one)]
    return tiles


def split(values):
    high = values.astype(jnp.bfloat16)
    return high, (values - high.astype(jnp.float32)).astype(jnp.bfloat16)


def turn_factors(turn, layer):
    pairs = [cos_sin(jnp.full((8, 128), turn[layer, g], jnp.float32)) for g in range(4)]
    return [c for c, _ in pairs], [s for _, s in pairs]


def store_tables(cos, sin, rest, bits, lanes_ref, rows_ref):
    col = lax.broadcasted_iota(jnp.int32, (8, 128), 1)
    sub = lax.broadcasted_iota(jnp.int32, (8, 128), 0)

    def pair(bit, cos, sin, back):
        one = ((col >> bit) & 1) == 1
        if back:
            return jnp.where(one, -sin, cos), jnp.where(one, cos, sin)
        return jnp.where(one, sin, cos), jnp.where(one, cos, -sin)

    def low(cos, sin, back):
        table = jnp.ones((8, 128), jnp.float32)
        for bit in range(3):
            zero, one = pair(bit, cos, sin, back)
            table = table * jnp.where(((sub >> bit) & 1) == 1, one, zero)
        return table

    tiles = kron(low(cos[0], sin[0], False) * rest, [pair(k, cos[0], sin[0], False) for k in (6, 5, 4, 3)])
    for k, t in enumerate(tiles):
        high, less = split(t)
        rows, more = slice(8 * k, 8 * k + 8), slice(128 + 8 * k, 136 + 8 * k)
        lanes_ref[rows, 0:128] = high
        lanes_ref[rows, 128:256] = less
        lanes_ref[more, 0:128] = high
        lanes_ref[more, 128:256] = jnp.zeros_like(high)
    tiles = low(cos[ROWS], sin[ROWS], True)
    g = bits[0]
    for half, top in enumerate(((cos[g], sin[g]), (-sin[g], cos[g]))):
        pairs = [pair(6 - k, cos[h], sin[h], True) for k, h in enumerate(bits[1:])]
        for k, t in enumerate(kron(tiles, [top] + pairs)):
            high, less = split(t)
            rows = slice(8 * k, 8 * k + 8)
            for third, part in enumerate((high, high, less)):
                at = 256 * third + 128 * half
                rows_ref[rows, at : at + 128] = part


def mix(parts, lanes_ref, rows_ref):
    rows = jnp.concatenate([t for tiles in parts for t in tiles], axis=0)
    both = jnp.dot(
        jnp.concatenate(split(rows), axis=1), lanes_ref[...], preferred_element_type=jnp.float32
    )
    high, low = split(both[:, 0:128] + both[:, 128:256])
    out = []
    for b in range(0, 256 * len(parts), 512):
        h, l = (jnp.concatenate([v[b : b + 256], v[b + 256 : b + 512]], axis=1) for v in (high, low))
        mixed = jnp.dot(
            rows_ref[...], jnp.concatenate([h, l, h], axis=0), preferred_element_type=jnp.float32
        )
        out += [[mixed[8 * i : 8 * i + 8, 128 * p : 128 * p + 128] for i in range(32)] for p in range(2)]
    return out


def in_step(prepare, finish, blocks):
    for k in range(5):
        now, last = blocks[k % 2], blocks[(k + 1) % 2]
        if k < 4:
            prepare(2 * k, now, 0)
            prepare(2 * k + 1, now, 1)
        if k:
            finish(2 * k - 2, last)


def mix_blocks(block, lanes, rows, held, b):
    parts = mix(
        [[block[at, p, i] for i in range(32)] for at in range(2) for p in range(2)], lanes, rows
    )
    for k, tiles in enumerate(parts):
        for i in range(32):
            held[k % 2, b + k // 2, i] = tiles[i]


def first_kernel(
    turn_hbm,
    angle_hbm,
    state_hbm,
    levels_hbm,
    out,
    tans,
    next_lanes,
    next_rows,
    turn,
    angle,
    state,
    lanes,
    rows,
    even,
    odd,
    sems,
):
    small = [
        pltpu.make_async_copy(turn_hbm, turn, sems.at[0]),
        pltpu.make_async_copy(angle_hbm, angle, sems.at[1]),
    ]
    copies = [
        (
            pltpu.make_async_copy(levels_hbm.at[b], out.at[b, :, 2], sems.at[2 + 2 * b]),
            pltpu.make_async_copy(state_hbm.at[:, b], state.at[:, b], sems.at[3 + 2 * b]),
        )
        for b in range(8)
    ]

    for c in small:
        c.start()
    for pair in copies:
        for c in pair:
            c.start()
    for c in small:
        c.wait()
    cos, sin = turn_factors(turn, 0)
    for g in range(1, 4):
        tans[g] = sin[g] / cos[g]
    block0 = tans[BLOCK]
    two, four = cos[BLOCK] * cos[BLOCK], cos[MIDDLE] * cos[MIDDLE]
    rest = two * two * two * four * four
    store_tables(cos, sin, rest, (BLOCK, ROWS, ROWS, ROWS, ROWS), lanes, rows)
    turned = jnp.broadcast_to(angle[0:1], (8, 128))

    def later_tables():
        cos, sin = turn_factors(turn, 1)
        for g in range(1, 4):
            tans[4 + g] = sin[g] / cos[g]
        pair = cos[ROWS] * cos[BLOCK]
        rest = pair * pair * pair * cos[BLOCK]
        for g in PLACE[:3]:
            rest = rest * cos[g]
        store_tables(cos, sin, rest, (*PLACE[3:], ROWS), next_lanes, next_rows)

    def prepare(b, block, at):
        if not at:
            for pair in copies[b : b + 2] if b < 2 else copies[2:] if b == 2 else ():
                for c in pair:
                    c.wait()
            if b == 4:
                later_tables()
        for i in range(32):
            level = out[b, i >> 1, 2, i & 1]
            block[at, 0, i], block[at, 1, i] = phase(state[0, b, i], state[1, b, i], level, turned)

    def finish(b, block):
        mix_blocks(block, lanes, rows, state, b)

    in_step(prepare, finish, (even, odd))

    @pl.loop(0, 32, unroll=4)
    def _(j):
        for p in range(2):
            tiles = rotate_all([state[p, i, j] for i in range(8)], [block0] * 3)
            for i in range(8):
                out[i, j >> 1, p, j & 1] = tiles[i]


def second_kernel(state, angle, tans, lanes, rows, out, held, even, odd):
    tans0, tans1 = ([tans[4 * layer + g] for g in PLACE] for layer in range(2))
    turned = jnp.broadcast_to(angle[1:2], (8, 128))

    @pl.loop(0, 32, unroll=4)
    def _(j):
        for p in range(2):
            tiles = rotate_all([state[i, j >> 1, p, j & 1] for i in range(8)], tans0[:3])
            for i in range(8):
                held[p, i, j] = tiles[i]

    def prepare(b, block, at):
        for r in range(2):
            re, im = (
                rotate_all([held[p, b, 2 * q + r] for q in range(16)], tans0[3:])
                for p in range(2)
            )
            for q in range(16):
                level = state[b, q, 2, r]
                i = 2 * q + r
                block[at, 0, i], block[at, 1, i] = phase(re[q], im[q], level, turned)

    def finish(b, block):
        mix_blocks(block, lanes, rows, held, b)

    in_step(prepare, finish, (even, odd))

    @pl.loop(0, 32, unroll=4)
    def _(j):
        for p in range(2):
            tiles = rotate_all([held[p, i, j] for i in range(8)], tans1[:3])
            for i in range(8):
                out[i, j >> 1, p, j & 1] = tiles[i]


def third_kernel(state, tans, out_hbm, held, done, sems):
    row, block = tans[4 + ROWS], tans[4 + BLOCK]
    copies = []
    for p in range(2):

        @pl.loop(0, 32, unroll=4)
        def _(j):
            tiles = rotate_all([state[i, j >> 1, p, j & 1] for i in range(8)], [block] * 3)
            for i in range(8):
                held[p, i, j] = tiles[i]

        for b in range(8):
            for r in range(2):
                tiles = rotate_all([held[p, b, 2 * q + r] for q in range(16)], [block, row, row, row])
                for q in range(16):
                    done[p, b, 2 * q + r] = tiles[q]
            copies.append(pltpu.make_async_copy(done.at[p, b], out_hbm.at[p, b], sems.at[8 * p + b]))
            copies[-1].start()
    for c in copies:
        c.wait()


def spec(space):
    return pl.BlockSpec(memory_space=space)


def call(kernel, name, shapes, ins, outs, inputs, scratch, flops, limit):
    return pl.pallas_call(
        kernel,
        out_shape=[jax.ShapeDtypeStruct(s, d) for s, d in shapes],
        in_specs=[spec(s) for s in ins],
        out_specs=[spec(s) for s in outs],
        scratch_shapes=list(scratch),
        name=name,
        cost_estimate=pl.CostEstimate(flops=flops, bytes_accessed=5 << 20, transcendentals=0),
        compiler_params=pltpu.CompilerParams(vmem_limit_bytes=limit << 20),
    )(*inputs)


def exchange(state, shape):
    flat = lax.all_to_all(state.reshape(128, -1, 128), ORDER, 0, 0, tiled=True)
    return flat.reshape(shape)


def body(amplitudes, energies, diagonal_angles, turn_angles):
    f32, bf16 = jnp.float32, jnp.bfloat16
    block = VMEM((2, 2, 32, 8, 128), f32)
    state, tans, lanes, rows = call(
        first_kernel,
        "first",
        [(SENT, f32), ((8, 8, 128), f32), ((256, 256), bf16), ((256, 768), bf16)],
        [pltpu.HBM] * 4,
        [VMEM] * 4,
        [
            pltpu.with_memory_space_constraint(a, pltpu.HBM)
            for a in (
                turn_angles,
                diagonal_angles,
                amplitudes.reshape(HOME),
                energies.reshape(8, 16, 2, 8, 128),
            )
        ],
        [
            SMEM((2, 4), f32),
            VMEM((2, 128), f32),
            VMEM(HOME, f32),
            VMEM((256, 256), bf16),
            VMEM((256, 768), bf16),
            block,
            block,
            pltpu.SemaphoreType.DMA((18,)),
        ],
        20_000_000,
        16,
    )
    state = exchange(state, SENT)
    (state,) = call(
        second_kernel,
        "second",
        [(AWAY, f32)],
        [VMEM] * 5,
        [VMEM],
        (state, diagonal_angles, tans, lanes, rows),
        [VMEM(HOME, f32), block, block],
        20_000_000,
        16,
    )
    state = exchange(state, AWAY)
    (state,) = call(
        third_kernel,
        "third",
        [(HOME, f32)],
        [VMEM] * 2,
        [pltpu.HBM],
        (state, tans),
        [VMEM(HOME, f32), VMEM(HOME, f32), pltpu.SemaphoreType.DMA((16,))],
        10_000_000,
        16,
    )
    return state.reshape(amplitudes.shape)


def solution(mesh):
    torus = Mesh(mesh.devices.reshape(4, 2, 4, 4), AXES)
    in_specs = (P(None, AXES, None, None), P(AXES, None, None), P(), P())
    out_specs = P(None, AXES, None, None)
    return jax.shard_map(body, mesh=torus, in_specs=in_specs, out_specs=out_specs, check_vma=False)
```

```python
import jax
import jax.numpy as jnp
import numpy as np
from jax import lax
from jax.experimental import pallas as pl
from jax.experimental.pallas import tpu as pltpu
from jax.sharding import Mesh
from jax.sharding import PartitionSpec as P

AXES = ("x", "c", "z", "y")
ORDER = ("z", "c", "y", "x")
VMEM = pltpu.VMEM
SMEM = pltpu.SMEM
HOME = (2, 8, 32, 8, 128)
SENT = (8, 16, 3, 2, 8, 128)
AWAY = (8, 16, 2, 2, 8, 128)
LANES, ROWS, BLOCK, MIDDLE = range(4)
PLACE = [g for a in ORDER for g in {"x": [BLOCK] * 2, "c": [BLOCK], "y": [MIDDLE] * 2, "z": [MIDDLE] * 2}[a]]


def fit(fn, terms, most=5.77):
    k = np.arange(400)
    s = most / 2 * (1 + np.cos(np.pi * (k + 0.5) / 400))
    series = np.polynomial.Chebyshev.fit(s, fn(np.sqrt(s)), terms - 1, domain=[0, most])
    return [float(c) for c in series.convert(kind=np.polynomial.Polynomial).coef]


SIN = fit(lambda t: np.sqrt(0.5) * np.sinc(t / 2 / np.pi), 4)


def horner(coef, s):
    total = s * coef[-1] + coef[-2]
    for c in coef[-3::-1]:
        total = total * s + c
    return total


def cos_sin(turn):
    half = horner(SIN, turn * turn) * turn
    cos = 1.0 - half * half
    above = 1.0 + cos
    return cos, half * above * lax.rsqrt(above)


def phase(re, im, level, angle):
    cos, sin = cos_sin(level * angle)
    return re * cos + im * sin, im * cos - re * sin


def rotate(tiles, bit, tan):
    step = 1 << bit
    out = list(tiles)
    for i, u in enumerate(tiles):
        if not i & step:
            v = tiles[i + step]
            out[i] = u - tan * v
            out[i + step] = v + tan * u
    return out


def rotate_all(tiles, tans):
    for bit, tan in zip(reversed(range(len(tans))), tans):
        tiles = rotate(tiles, bit, tan)
    return tiles


def kron(columns, pairs):
    tiles = [columns]
    for zero, one in pairs:
        tiles = [t * f for t in tiles for f in (zero, one)]
    return tiles


def split(values):
    high = values.astype(jnp.bfloat16)
    return high, (values - high.astype(jnp.float32)).astype(jnp.bfloat16)


def turn_factors(turn, layer):
    pairs = [cos_sin(jnp.full((8, 128), turn[layer, g], jnp.float32)) for g in range(4)]
    return [c for c, _ in pairs], [s for _, s in pairs]


def store_tables(cos, sin, rest, bits, lanes_ref, rows_ref):
    col = lax.broadcasted_iota(jnp.int32, (8, 128), 1)
    sub = lax.broadcasted_iota(jnp.int32, (8, 128), 0)

    def pair(bit, cos, sin, back):
        one = ((col >> bit) & 1) == 1
        if back:
            return jnp.where(one, -sin, cos), jnp.where(one, cos, sin)
        return jnp.where(one, sin, cos), jnp.where(one, cos, -sin)

    def low(cos, sin, back):
        table = jnp.ones((8, 128), jnp.float32)
        for bit in range(3):
            zero, one = pair(bit, cos, sin, back)
            table = table * jnp.where(((sub >> bit) & 1) == 1, one, zero)
        return table

    tiles = kron(low(cos[0], sin[0], False) * rest, [pair(k, cos[0], sin[0], False) for k in (6, 5, 4, 3)])
    for k, t in enumerate(tiles):
        high, less = split(t)
        rows, more = slice(8 * k, 8 * k + 8), slice(128 + 8 * k, 136 + 8 * k)
        lanes_ref[rows, 0:128] = high
        lanes_ref[rows, 128:256] = less
        lanes_ref[more, 0:128] = high
        lanes_ref[more, 128:256] = jnp.zeros_like(high)
    tiles = low(cos[ROWS], sin[ROWS], True)
    g = bits[0]
    for half, top in enumerate(((cos[g], sin[g]), (-sin[g], cos[g]))):
        pairs = [pair(6 - k, cos[h], sin[h], True) for k, h in enumerate(bits[1:])]
        for k, t in enumerate(kron(tiles, [top] + pairs)):
            high, less = split(t)
            rows = slice(8 * k, 8 * k + 8)
            for third, part in enumerate((high, high, less)):
                at = 256 * third + 128 * half
                rows_ref[rows, at : at + 128] = part


def mix(parts, lanes_ref, rows_ref):
    rows = jnp.concatenate([t for tiles in parts for t in tiles], axis=0)
    both = jnp.dot(
        jnp.concatenate(split(rows), axis=1), lanes_ref[...], preferred_element_type=jnp.float32
    )
    high, low = split(both[:, 0:128] + both[:, 128:256])
    out = []
    for b in range(0, 256 * len(parts), 512):
        h, l = (jnp.concatenate([v[b : b + 256], v[b + 256 : b + 512]], axis=1) for v in (high, low))
        mixed = jnp.dot(
            rows_ref[...], jnp.concatenate([h, l, h], axis=0), preferred_element_type=jnp.float32
        )
        out += [[mixed[8 * i : 8 * i + 8, 128 * p : 128 * p + 128] for i in range(32)] for p in range(2)]
    return out


def in_step(prepare, finish, blocks):
    for k in range(5):
        now, last = blocks[k % 2], blocks[(k + 1) % 2]
        if k < 4:
            prepare(2 * k, now, 0)
            prepare(2 * k + 1, now, 1)
        if k:
            finish(2 * k - 2, last)


def mix_blocks(block, lanes, rows, held, b):
    parts = mix(
        [[block[at, p, i] for i in range(32)] for at in range(2) for p in range(2)], lanes, rows
    )
    for k, tiles in enumerate(parts):
        for i in range(32):
            held[k % 2, b + k // 2, i] = tiles[i]


def first_kernel(
    turn_hbm,
    angle_hbm,
    state_hbm,
    levels_hbm,
    out,
    tans,
    next_lanes,
    next_rows,
    turn,
    angle,
    state,
    lanes,
    rows,
    even,
    odd,
    sems,
):
    small = [
        pltpu.make_async_copy(turn_hbm, turn, sems.at[0]),
        pltpu.make_async_copy(angle_hbm, angle, sems.at[1]),
    ]
    copies = [
        (
            pltpu.make_async_copy(levels_hbm.at[b], out.at[b, :, 2], sems.at[2 + 2 * b]),
            pltpu.make_async_copy(state_hbm.at[:, b], state.at[:, b], sems.at[3 + 2 * b]),
        )
        for b in range(8)
    ]

    for c in small:
        c.start()
    for pair in copies:
        for c in pair:
            c.start()
    for c in small:
        c.wait()
    cos, sin = turn_factors(turn, 0)
    for g in range(1, 4):
        tans[g] = sin[g] / cos[g]
    block0 = tans[BLOCK]
    two, four = cos[BLOCK] * cos[BLOCK], cos[MIDDLE] * cos[MIDDLE]
    rest = two * two * two * four * four
    store_tables(cos, sin, rest, (BLOCK, ROWS, ROWS, ROWS, ROWS), lanes, rows)
    turned = jnp.broadcast_to(angle[0:1], (8, 128))

    def later_tables():
        cos, sin = turn_factors(turn, 1)
        for g in range(1, 4):
            tans[4 + g] = sin[g] / cos[g]
        pair = cos[ROWS] * cos[BLOCK]
        rest = pair * pair * pair * cos[BLOCK]
        for g in PLACE[:3]:
            rest = rest * cos[g]
        store_tables(cos, sin, rest, (*PLACE[3:], ROWS), next_lanes, next_rows)

    def prepare(b, block, at):
        if not at:
            for pair in copies[b : b + 2] if b < 2 else copies[2:] if b == 2 else ():
                for c in pair:
                    c.wait()
            if b == 4:
                later_tables()
        for i in range(32):
            level = out[b, i >> 1, 2, i & 1]
            block[at, 0, i], block[at, 1, i] = phase(state[0, b, i], state[1, b, i], level, turned)

    def finish(b, block):
        mix_blocks(block, lanes, rows, state, b)

    in_step(prepare, finish, (even, odd))

    @pl.loop(0, 32, unroll=8)
    def _(j):
        for p in range(2):
            tiles = rotate_all([state[p, i, j] for i in range(8)], [block0] * 3)
            for i in range(8):
                out[i, j >> 1, p, j & 1] = tiles[i]


def second_kernel(state, angle, tans, lanes, rows, out, held, even, odd):
    tans0, tans1 = ([tans[4 * layer + g] for g in PLACE] for layer in range(2))
    turned = jnp.broadcast_to(angle[1:2], (8, 128))

    @pl.loop(0, 32, unroll=8)
    def _(j):
        for p in range(2):
            tiles = rotate_all([state[i, j >> 1, p, j & 1] for i in range(8)], tans0[:3])
            for i in range(8):
                held[p, i, j] = tiles[i]

    def prepare(b, block, at):
        for r in range(2):
            re, im = (
                rotate_all([held[p, b, 2 * q + r] for q in range(16)], tans0[3:])
                for p in range(2)
            )
            for q in range(16):
                level = state[b, q, 2, r]
                i = 2 * q + r
                block[at, 0, i], block[at, 1, i] = phase(re[q], im[q], level, turned)

    def finish(b, block):
        mix_blocks(block, lanes, rows, held, b)

    in_step(prepare, finish, (even, odd))

    @pl.loop(0, 32, unroll=8)
    def _(j):
        for p in range(2):
            tiles = rotate_all([held[p, i, j] for i in range(8)], tans1[:3])
            for i in range(8):
                out[i, j >> 1, p, j & 1] = tiles[i]


def third_kernel(state, tans, out_hbm, held, done, sems):
    row, block = tans[4 + ROWS], tans[4 + BLOCK]
    copies = []
    for p in range(2):

        @pl.loop(0, 32, unroll=8)
        def _(j):
            tiles = rotate_all([state[i, j >> 1, p, j & 1] for i in range(8)], [block] * 3)
            for i in range(8):
                held[p, i, j] = tiles[i]

        for b in range(8):
            for r in range(2):
                tiles = rotate_all([held[p, b, 2 * q + r] for q in range(16)], [block, row, row, row])
                for q in range(16):
                    done[p, b, 2 * q + r] = tiles[q]
            copies.append(pltpu.make_async_copy(done.at[p, b], out_hbm.at[p, b], sems.at[8 * p + b]))
            copies[-1].start()
    for c in copies:
        c.wait()


def spec(space):
    return pl.BlockSpec(memory_space=space)


def call(kernel, name, shapes, ins, outs, inputs, scratch, flops, limit):
    return pl.pallas_call(
        kernel,
        out_shape=[jax.ShapeDtypeStruct(s, d) for s, d in shapes],
        in_specs=[spec(s) for s in ins],
        out_specs=[spec(s) for s in outs],
        scratch_shapes=list(scratch),
        name=name,
        cost_estimate=pl.CostEstimate(flops=flops, bytes_accessed=5 << 20, transcendentals=0),
        compiler_params=pltpu.CompilerParams(vmem_limit_bytes=limit << 20),
    )(*inputs)


def exchange(state, shape):
    flat = lax.all_to_all(state.reshape(128, -1, 128), ORDER, 0, 0, tiled=True)
    return flat.reshape(shape)


def body(amplitudes, energies, diagonal_angles, turn_angles):
    f32, bf16 = jnp.float32, jnp.bfloat16
    block = VMEM((2, 2, 32, 8, 128), f32)
    state, tans, lanes, rows = call(
        first_kernel,
        "first",
        [(SENT, f32), ((8, 8, 128), f32), ((256, 256), bf16), ((256, 768), bf16)],
        [pltpu.HBM] * 4,
        [VMEM] * 4,
        [
            pltpu.with_memory_space_constraint(a, pltpu.HBM)
            for a in (
                turn_angles,
                diagonal_angles,
                amplitudes.reshape(HOME),
                energies.reshape(8, 16, 2, 8, 128),
            )
        ],
        [
            SMEM((2, 4), f32),
            VMEM((2, 128), f32),
            VMEM(HOME, f32),
            VMEM((256, 256), bf16),
            VMEM((256, 768), bf16),
            block,
            block,
            pltpu.SemaphoreType.DMA((18,)),
        ],
        20_000_000,
        16,
    )
    state = exchange(state, SENT)
    (state,) = call(
        second_kernel,
        "second",
        [(AWAY, f32)],
        [VMEM] * 5,
        [VMEM],
        (state, diagonal_angles, tans, lanes, rows),
        [VMEM(HOME, f32), block, block],
        20_000_000,
        16,
    )
    state = exchange(state, AWAY)
    (state,) = call(
        third_kernel,
        "third",
        [(HOME, f32)],
        [VMEM] * 2,
        [pltpu.HBM],
        (state, tans),
        [VMEM(HOME, f32), VMEM(HOME, f32), pltpu.SemaphoreType.DMA((16,))],
        10_000_000,
        16,
    )
    return state.reshape(amplitudes.shape)


def solution(mesh):
    torus = Mesh(mesh.devices.reshape(4, 2, 4, 4), AXES)
    in_specs = (P(None, AXES, None, None), P(AXES, None, None), P(), P())
    out_specs = P(None, AXES, None, None)
    return jax.shard_map(body, mesh=torus, in_specs=in_specs, out_specs=out_specs, check_vma=False)
```

```python
import jax
import jax.numpy as jnp
import numpy as np
from jax import lax
from jax.experimental import pallas as pl
from jax.experimental.pallas import tpu as pltpu
from jax.sharding import Mesh
from jax.sharding import PartitionSpec as P

AXES = ("x", "c", "z", "y")
ORDER = ("y", "c", "z", "x")
VMEM = pltpu.VMEM
SMEM = pltpu.SMEM
HOME = (2, 8, 32, 8, 128)
SENT = (8, 16, 3, 2, 8, 128)
AWAY = (8, 16, 2, 2, 8, 128)
LANES, ROWS, BLOCK, MIDDLE = range(4)
PLACE = [g for a in ORDER for g in {"x": [BLOCK] * 2, "c": [BLOCK], "y": [MIDDLE] * 2, "z": [MIDDLE] * 2}[a]]


def fit(fn, terms, most=5.77):
    k = np.arange(400)
    s = most / 2 * (1 + np.cos(np.pi * (k + 0.5) / 400))
    series = np.polynomial.Chebyshev.fit(s, fn(np.sqrt(s)), terms - 1, domain=[0, most])
    return [float(c) for c in series.convert(kind=np.polynomial.Polynomial).coef]


SIN = fit(lambda t: np.sqrt(0.5) * np.sinc(t / 2 / np.pi), 4)


def horner(coef, s):
    total = s * coef[-1] + coef[-2]
    for c in coef[-3::-1]:
        total = total * s + c
    return total


def cos_sin(turn):
    half = horner(SIN, turn * turn) * turn
    cos = 1.0 - half * half
    above = 1.0 + cos
    return cos, half * above * lax.rsqrt(above)


def phase(re, im, level, angle):
    cos, sin = cos_sin(level * angle)
    return re * cos + im * sin, im * cos - re * sin


def rotate(tiles, bit, tan):
    step = 1 << bit
    out = list(tiles)
    for i, u in enumerate(tiles):
        if not i & step:
            v = tiles[i + step]
            out[i] = u - tan * v
            out[i + step] = v + tan * u
    return out


def rotate_all(tiles, tans):
    for bit, tan in zip(reversed(range(len(tans))), tans):
        tiles = rotate(tiles, bit, tan)
    return tiles


def kron(columns, pairs):
    tiles = [columns]
    for zero, one in pairs:
        tiles = [t * f for t in tiles for f in (zero, one)]
    return tiles


def split(values):
    high = values.astype(jnp.bfloat16)
    return high, (values - high.astype(jnp.float32)).astype(jnp.bfloat16)


def turn_factors(turn, layer):
    pairs = [cos_sin(jnp.full((8, 128), turn[layer, g], jnp.float32)) for g in range(4)]
    return [c for c, _ in pairs], [s for _, s in pairs]


def store_tables(cos, sin, rest, bits, lanes_ref, rows_ref):
    col = lax.broadcasted_iota(jnp.int32, (8, 128), 1)
    sub = lax.broadcasted_iota(jnp.int32, (8, 128), 0)

    def pair(bit, cos, sin, back):
        one = ((col >> bit) & 1) == 1
        if back:
            return jnp.where(one, -sin, cos), jnp.where(one, cos, sin)
        return jnp.where(one, sin, cos), jnp.where(one, cos, -sin)

    def low(cos, sin, back):
        table = jnp.ones((8, 128), jnp.float32)
        for bit in range(3):
            zero, one = pair(bit, cos, sin, back)
            table = table * jnp.where(((sub >> bit) & 1) == 1, one, zero)
        return table

    tiles = kron(low(cos[0], sin[0], False) * rest, [pair(k, cos[0], sin[0], False) for k in (6, 5, 4, 3)])
    for k, t in enumerate(tiles):
        high, less = split(t)
        rows, more = slice(8 * k, 8 * k + 8), slice(128 + 8 * k, 136 + 8 * k)
        lanes_ref[rows, 0:128] = high
        lanes_ref[rows, 128:256] = less
        lanes_ref[more, 0:128] = high
        lanes_ref[more, 128:256] = jnp.zeros_like(high)
    tiles = low(cos[ROWS], sin[ROWS], True)
    g = bits[0]
    for half, top in enumerate(((cos[g], sin[g]), (-sin[g], cos[g]))):
        pairs = [pair(6 - k, cos[h], sin[h], True) for k, h in enumerate(bits[1:])]
        for k, t in enumerate(kron(tiles, [top] + pairs)):
            high, less = split(t)
            rows = slice(8 * k, 8 * k + 8)
            for third, part in enumerate((high, high, less)):
                at = 256 * third + 128 * half
                rows_ref[rows, at : at + 128] = part


def mix(parts, lanes_ref, rows_ref):
    rows = jnp.concatenate([t for tiles in parts for t in tiles], axis=0)
    both = jnp.dot(
        jnp.concatenate(split(rows), axis=1), lanes_ref[...], preferred_element_type=jnp.float32
    )
    high, low = split(both[:, 0:128] + both[:, 128:256])
    out = []
    for b in range(0, 256 * len(parts), 512):
        h, l = (jnp.concatenate([v[b : b + 256], v[b + 256 : b + 512]], axis=1) for v in (high, low))
        mixed = jnp.dot(
            rows_ref[...], jnp.concatenate([h, l, h], axis=0), preferred_element_type=jnp.float32
        )
        out += [[mixed[8 * i : 8 * i + 8, 128 * p : 128 * p + 128] for i in range(32)] for p in range(2)]
    return out


def in_step(prepare, finish, blocks):
    for k in range(5):
        now, last = blocks[k % 2], blocks[(k + 1) % 2]
        if k < 4:
            prepare(2 * k, now, 0)
            prepare(2 * k + 1, now, 1)
        if k:
            finish(2 * k - 2, last)


def mix_blocks(block, lanes, rows, held, b):
    parts = mix(
        [[block[at, p, i] for i in range(32)] for at in range(2) for p in range(2)], lanes, rows
    )
    for k, tiles in enumerate(parts):
        for i in range(32):
            held[k % 2, b + k // 2, i] = tiles[i]


def first_kernel(
    turn_hbm,
    angle_hbm,
    state_hbm,
    levels_hbm,
    out,
    tans,
    next_lanes,
    next_rows,
    turn,
    angle,
    state,
    lanes,
    rows,
    even,
    odd,
    sems,
):
    small = [
        pltpu.make_async_copy(turn_hbm, turn, sems.at[0]),
        pltpu.make_async_copy(angle_hbm, angle, sems.at[1]),
    ]
    copies = [
        (
            pltpu.make_async_copy(levels_hbm.at[b], out.at[b, :, 2], sems.at[2 + 2 * b]),
            pltpu.make_async_copy(state_hbm.at[:, b], state.at[:, b], sems.at[3 + 2 * b]),
        )
        for b in range(8)
    ]

    for c in small:
        c.start()
    for pair in copies:
        for c in pair:
            c.start()
    for c in small:
        c.wait()
    cos, sin = turn_factors(turn, 0)
    for g in range(1, 4):
        tans[g] = sin[g] / cos[g]
    block0 = tans[BLOCK]
    two, four = cos[BLOCK] * cos[BLOCK], cos[MIDDLE] * cos[MIDDLE]
    rest = two * two * two * four * four
    store_tables(cos, sin, rest, (BLOCK, ROWS, ROWS, ROWS, ROWS), lanes, rows)
    turned = jnp.broadcast_to(angle[0:1], (8, 128))

    def later_tables():
        cos, sin = turn_factors(turn, 1)
        for g in range(1, 4):
            tans[4 + g] = sin[g] / cos[g]
        pair = cos[ROWS] * cos[BLOCK]
        rest = pair * pair * pair * cos[BLOCK]
        for g in PLACE[:3]:
            rest = rest * cos[g]
        store_tables(cos, sin, rest, (*PLACE[3:], ROWS), next_lanes, next_rows)

    def prepare(b, block, at):
        if not at:
            for pair in copies[b : b + 2] if b < 2 else copies[2:] if b == 2 else ():
                for c in pair:
                    c.wait()
            if b == 4:
                later_tables()
        for i in range(32):
            level = out[b, i >> 1, 2, i & 1]
            block[at, 0, i], block[at, 1, i] = phase(state[0, b, i], state[1, b, i], level, turned)

    def finish(b, block):
        mix_blocks(block, lanes, rows, state, b)

    in_step(prepare, finish, (even, odd))

    @pl.loop(0, 32, unroll=8)
    def _(j):
        for p in range(2):
            tiles = rotate_all([state[p, i, j] for i in range(8)], [block0] * 3)
            for i in range(8):
                out[i, j >> 1, p, j & 1] = tiles[i]


def second_kernel(state, angle, tans, lanes, rows, out, held, even, odd):
    tans0, tans1 = ([tans[4 * layer + g] for g in PLACE] for layer in range(2))
    turned = jnp.broadcast_to(angle[1:2], (8, 128))

    @pl.loop(0, 32, unroll=8)
    def _(j):
        for p in range(2):
            tiles = rotate_all([state[i, j >> 1, p, j & 1] for i in range(8)], tans0[:3])
            for i in range(8):
                held[p, i, j] = tiles[i]

    def prepare(b, block, at):
        for r in range(2):
            re, im = (
                rotate_all([held[p, b, 2 * q + r] for q in range(16)], tans0[3:])
                for p in range(2)
            )
            for q in range(16):
                level = state[b, q, 2, r]
                i = 2 * q + r
                block[at, 0, i], block[at, 1, i] = phase(re[q], im[q], level, turned)

    def finish(b, block):
        mix_blocks(block, lanes, rows, held, b)

    in_step(prepare, finish, (even, odd))

    @pl.loop(0, 32, unroll=8)
    def _(j):
        for p in range(2):
            tiles = rotate_all([held[p, i, j] for i in range(8)], tans1[:3])
            for i in range(8):
                out[i, j >> 1, p, j & 1] = tiles[i]


def third_kernel(state, tans, out_hbm, held, done, sems):
    row, block = tans[4 + ROWS], tans[4 + BLOCK]
    copies = []
    for p in range(2):

        @pl.loop(0, 32, unroll=8)
        def _(j):
            tiles = rotate_all([state[i, j >> 1, p, j & 1] for i in range(8)], [block] * 3)
            for i in range(8):
                held[p, i, j] = tiles[i]

        for b in range(8):
            for r in range(2):
                tiles = rotate_all([held[p, b, 2 * q + r] for q in range(16)], [block, row, row, row])
                for q in range(16):
                    done[p, b, 2 * q + r] = tiles[q]
            copies.append(pltpu.make_async_copy(done.at[p, b], out_hbm.at[p, b], sems.at[8 * p + b]))
            copies[-1].start()
    for c in copies:
        c.wait()


def spec(space):
    return pl.BlockSpec(memory_space=space)


def call(kernel, name, shapes, ins, outs, inputs, scratch, flops, limit):
    return pl.pallas_call(
        kernel,
        out_shape=[jax.ShapeDtypeStruct(s, d) for s, d in shapes],
        in_specs=[spec(s) for s in ins],
        out_specs=[spec(s) for s in outs],
        scratch_shapes=list(scratch),
        name=name,
        cost_estimate=pl.CostEstimate(flops=flops, bytes_accessed=5 << 20, transcendentals=0),
        compiler_params=pltpu.CompilerParams(vmem_limit_bytes=limit << 20),
    )(*inputs)


def exchange(state, shape):
    flat = lax.all_to_all(state.reshape(128, -1, 128), ORDER, 0, 0, tiled=True)
    return flat.reshape(shape)


def body(amplitudes, energies, diagonal_angles, turn_angles):
    f32, bf16 = jnp.float32, jnp.bfloat16
    block = VMEM((2, 2, 32, 8, 128), f32)
    state, tans, lanes, rows = call(
        first_kernel,
        "first",
        [(SENT, f32), ((8, 8, 128), f32), ((256, 256), bf16), ((256, 768), bf16)],
        [pltpu.HBM] * 4,
        [VMEM] * 4,
        [
            pltpu.with_memory_space_constraint(a, pltpu.HBM)
            for a in (
                turn_angles,
                diagonal_angles,
                amplitudes.reshape(HOME),
                energies.reshape(8, 16, 2, 8, 128),
            )
        ],
        [
            SMEM((2, 4), f32),
            VMEM((2, 128), f32),
            VMEM(HOME, f32),
            VMEM((256, 256), bf16),
            VMEM((256, 768), bf16),
            block,
            block,
            pltpu.SemaphoreType.DMA((18,)),
        ],
        20_000_000,
        16,
    )
    state = exchange(state, SENT)
    (state,) = call(
        second_kernel,
        "second",
        [(AWAY, f32)],
        [VMEM] * 5,
        [VMEM],
        (state, diagonal_angles, tans, lanes, rows),
        [VMEM(HOME, f32), block, block],
        20_000_000,
        16,
    )
    state = exchange(state, AWAY)
    (state,) = call(
        third_kernel,
        "third",
        [(HOME, f32)],
        [VMEM] * 2,
        [pltpu.HBM],
        (state, tans),
        [VMEM(HOME, f32), VMEM(HOME, f32), pltpu.SemaphoreType.DMA((16,))],
        10_000_000,
        16,
    )
    return state.reshape(amplitudes.shape)


def solution(mesh):
    torus = Mesh(mesh.devices.reshape(4, 2, 4, 4), AXES)
    in_specs = (P(None, AXES, None, None), P(AXES, None, None), P(), P())
    out_specs = P(None, AXES, None, None)
    return jax.shard_map(body, mesh=torus, in_specs=in_specs, out_specs=out_specs, check_vma=False)
```
